512 devices in a mesh: dp: 32 (over z, core), vocab: 16 (over y, x).
Axes of the slice: x: 4, y: 4, z: 16, core: 2. Of those that a mesh axis runs over, the one named last changes fastest.
Arguments:
- hidden: float32 [64, 2, 32, 4096], P('dp', None, None, 'vocab'), may hold values from -64 to 64, as said below
- head_weight: float32 [4096, 4096], P(None, 'vocab'), may hold values from -1 to 1, as said below
- targets: int32 [64, 2, 32], P('dp'), may hold values from 0 to 4095
- lengths: int32 [64, 2], P('dp'), may hold values from 8 to 32
- rest_lse: float32 [64, 2, 32], P('dp'), may hold values from 6 to 10
- ref_logp: float32 [64, 2], P('dp'), may hold values from -120 to 120
- group_map: int32 [64], P('dp'), may hold values from 0 to 31, as said below
- group_weight: float32 [32], replicated, may hold values from 0.25 to 4
Outputs:
- hidden_grad: float32 [64, 2, 32, 4096], P('dp', None, None, 'vocab')
- dpo_loss: float32 [], replicated
The draws below stay inside these ranges and needn't reach their ends.
Inputs may be any that keep to these rules, and one draw needn't show every extreme that they name: `hidden`: standard normal states; in some draws a few tokens lie near large multiples of two head columns. `head_weight`: entries of order one over the square root of 4096. `group_map`: each pair names its own group or one of the two next to it (indices modulo 32); every group is named by exactly 2 pairs, and at most one pair of a group names each neighbour.
All inputs are finite; a program needn't handle non-finite values.
Results may differ from the reference program's by a relative error of at most 0.0003.
Values sent between devices are 32-bit elements; how exact they have to be, the bound alone decides.
No kernel may reach another device: no remote copies, remote signals or barrier semaphores. Data moves between devices by JAX's collectives and lax.ppermute only.
A program may use at most 64 MiB of HBM per device.

```python
import math
import jax
import jax.numpy as jnp
import numpy as np
from jax import lax

D = 4096
SEQ = 32
PAIR_DEV = 2
WINDOW = 4096
PAIRS = 64
GROUPS = 32


def shared_draw(key):
    weight_key = jax.random.fold_in(key, 11)
    state_key = jax.random.fold_in(key, 12)
    weight = jax.random.truncated_normal(weight_key, -6.0, 6.0, (D, WINDOW), jnp.float32) / jnp.sqrt(jnp.float32(D))
    states = jax.random.truncated_normal(state_key, -6.0, 6.0, (PAIRS, 2, SEQ, D), jnp.float32)
    return (weight, states)


def draw_hidden(key, part):
    return shared_draw(key)[1]


def draw_head_weight(key, part):
    return shared_draw(key)[0]


def draw_group_map(key, part):
    swap_key = jax.random.fold_in(key, 21)
    order_key = jax.random.fold_in(key, 22)
    swaps = jax.random.randint(swap_key, (GROUPS,), 0, 2)
    group_ids = lax.iota(jnp.int32, GROUPS)
    going_left = jnp.roll(swaps, 1)
    scores = jax.random.randint(order_key, (GROUPS, PAIR_DEV), 0, 1 << 20) * PAIR_DEV + lax.iota(jnp.int32, PAIR_DEV)[None, :]
    ranking = jnp.argsort(jnp.argsort(scores, axis=1), axis=1).astype(jnp.int32)
    to_left = ranking < going_left[:, None]
    to_right = (ranking >= going_left[:, None]) & (ranking < (going_left + swaps)[:, None])
    left_group = (group_ids + GROUPS - 1) % GROUPS
    right_group = (group_ids + 1) % GROUPS
    target_group = jnp.where(to_left, left_group[:, None], jnp.where(to_right, right_group[:, None], group_ids[:, None]))
    return target_group.reshape(GROUPS * PAIR_DEV).astype(jnp.int32)


def plant(values, key, low, high):
    spot = [jax.random.randint(jax.random.fold_in(key, axis), (), 0, length) for axis, length in enumerate(values.shape)]
    longest = values.shape.index(max(values.shape))
    neighbour = spot[:longest] + [(spot[longest] + 1) % values.shape[longest]] + spot[longest + 1:]
    return values.at[tuple(spot)].set(low).at[tuple(neighbour)].set(high)


def levels(key, dims, cuts, least, top_value):
    gain, own = 1.0, jax.random.fold_in(key, 6)
    for axis_at, parts in cuts:
        draws = jnp.exp(jax.random.uniform(jax.random.fold_in(own, axis_at), (parts,), jnp.float32, least / len(cuts), top_value / len(cuts)))
        gain = gain * jnp.repeat(draws, dims[axis_at] // parts).reshape([-1 if axis == axis_at else 1 for axis in range(len(dims))])
    return gain


def rank_bounds(amount, lean):
    loads = [(1 << 20) // math.isqrt(rank ** lean) + 1 for rank in range(1, amount + 1)]
    deviation = 1 + sum(loads) // (1 << 30)
    return np.cumsum(np.array([max(1, weight // deviation) for weight in loads]))


def ranked_ids(own_key, extent, amount, lean):
    table = rank_bounds(amount, lean)
    ticket = jax.random.randint(jax.random.fold_in(own_key, 1), extent, 0, int(table[amount - 1]))
    standing = jnp.searchsorted(jnp.asarray(table, jnp.int32), ticket, side="right")
    return jax.random.permutation(jax.random.fold_in(own_key, 2), amount)[standing].astype(jnp.int32)


def noise(own_key, shape, deviation, bound, shards=(), held_as=jnp.bfloat16):
    gain = levels(own_key, shape, shards, -0.22, 0.18) if shards else 1.0
    values = jax.random.normal(own_key, shape, jnp.float32) * deviation * gain
    return jnp.minimum(jnp.maximum(values, -bound), bound).astype(held_as)


def setup_inputs(seed: int = 0) -> dict:
    splits = jax.random.split(jax.random.key(seed), 9)
    return {
        "hidden": draw_hidden(jax.random.fold_in(splits[8], 71), 0),
        "head_weight": draw_head_weight(jax.random.fold_in(splits[8], 71), 0),
        "targets": plant(ranked_ids(splits[2], (PAIRS, 2, SEQ), WINDOW, 2), jax.random.fold_in(splits[2], 3), 0, WINDOW - 1).astype(jnp.int32),
        "lengths": plant(jax.random.randint(splits[3], (PAIRS, 2), SEQ // 4, SEQ + 1), jax.random.fold_in(splits[3], 1), SEQ // 4, SEQ).astype(jnp.int32),
        "rest_lse": jnp.clip(6.0 + 4.0 * jax.random.uniform(splits[4], (PAIRS, 2, SEQ), jnp.float32) ** levels(splits[4], (PAIRS, 2, SEQ), ((0, 32),), -0.2, 0.2), 6.0, 10.0),
        "ref_logp": noise(splits[5], (PAIRS, 2), 20.0, 120.0, ((0, 32),), jnp.float32),
        "group_map": draw_group_map(jax.random.fold_in(splits[8], 71), 0),
        "group_weight": jnp.clip(jnp.exp(jax.random.uniform(splits[7], (GROUPS,), jnp.float32, math.log(0.25), math.log(4.0))), 0.25, 4.0),
    }


beta_scale = 0.05
highest = lax.Precision.HIGHEST


def reference(hidden, head_weight, targets, lengths, rest_lse, ref_logp, group_map, group_weight):
    token_rows = hidden.reshape(PAIRS * 2 * SEQ, D)
    logits = jnp.dot(token_rows, head_weight, precision=highest, preferred_element_type=jnp.float32)
    row_peak = jnp.max(logits, axis=1)
    row_total = jnp.sum(jnp.exp(logits - row_peak[:, None]), axis=1)
    window_lse = row_peak + jnp.log(row_total)
    target_flat = targets.reshape(PAIRS * 2 * SEQ)
    matches = target_flat[:, None] == lax.iota(jnp.int32, WINDOW)[None, :]
    target_logit = jnp.sum(jnp.where(matches, logits, 0.0), axis=1)
    outside = rest_lse.reshape(PAIRS * 2 * SEQ)
    ceiling = jnp.maximum(window_lse, outside)
    full_lse = ceiling + jnp.log(jnp.exp(window_lse - ceiling) + jnp.exp(outside - ceiling))
    positions = lax.iota(jnp.int32, SEQ)
    live_tokens = (positions[None, None, :] < lengths[:, :, None]).astype(jnp.float32)
    token_logp = (target_logit - full_lse).reshape(PAIRS, 2, SEQ) * live_tokens
    sequence_logp = jnp.sum(token_logp, axis=2)
    margin = beta_scale * ((sequence_logp[:, 0] - ref_logp[:, 0]) - (sequence_logp[:, 1] - ref_logp[:, 1]))
    group_ids = lax.iota(jnp.int32, GROUPS)
    pair_weight = jnp.sum(jnp.where(group_map[:, None] == group_ids[None, :], group_weight[None, :], 0.0), axis=1)
    divisor = PAIR_DEV * jnp.sum(group_weight)
    dpo_loss = jnp.sum(pair_weight * jax.nn.softplus(-margin)) / divisor
    coefficient = -beta_scale * pair_weight * jax.nn.sigmoid(-margin) / divisor
    sign_pair = jnp.array([1.0, -1.0], jnp.float32)
    token_grad = (coefficient[:, None, None] * sign_pair[None, :, None] * live_tokens).reshape(PAIRS * 2 * SEQ)
    probability = jnp.exp(logits - full_lse[:, None])
    logit_grad = token_grad[:, None] * (matches.astype(jnp.float32) - probability)
    hidden_grad = jnp.dot(logit_grad, head_weight.T, precision=highest, preferred_element_type=jnp.float32)
    return hidden_grad.reshape(PAIRS, 2, SEQ, D), dpo_loss
```

```python
import jax
import jax.numpy as jnp
from jax import lax
from jax.sharding import PartitionSpec as P

beta_scale = 0.05
logit_precision = lax.Precision.HIGH
grad_precision = lax.Precision.HIGH


def exchanged(blocks, axis):
    return lax.all_to_all(blocks, axis, split_axis=0, concat_axis=0, tiled=True)


def copies_from_all(shard, axis):
    return exchanged(jnp.broadcast_to(shard, (lax.axis_size(axis), *shard.shape)), axis)


def summed_by_swaps(value, axis):
    size = lax.axis_size(axis)
    step = 1
    while step < size:
        pairs = [(place, place ^ step) for place in range(size)]
        value = value + lax.ppermute(value, axis, pairs)
        step *= 2
    return value


def shards(hidden, head_weight, targets, lengths, rest_lse, ref_logp, group_map, group_weight):
    pair_count, _, seq_slots, local_width = hidden.shape
    column_count = head_weight.shape[1]
    holders = lax.axis_size("vocab")
    tokens = pair_count * 2 * seq_slots
    weight_blocks = head_weight.reshape(holders, local_width, column_count)
    states = copies_from_all(hidden.reshape(tokens, local_width), "vocab")

    column_ids = lax.axis_index("vocab") * column_count + lax.iota(jnp.int32, column_count)
    matches = targets.reshape(tokens)[:, None] == column_ids[None, :]
    logits = jnp.einsum(
        "vtf,vfc->tc",
        states,
        weight_blocks,
        precision=logit_precision,
        preferred_element_type=jnp.float32,
    )
    local_peak = jnp.max(logits, axis=1)
    scaled = jnp.exp(logits - local_peak[:, None])
    local_total = jnp.sum(scaled, axis=1)
    local_target = jnp.sum(jnp.where(matches, logits, 0.0), axis=1)
    stats = copies_from_all(jnp.stack([local_peak, local_total, local_target]), "vocab")
    both_rows = jnp.einsum(
        "tc,vfc->vtf",
        jnp.concatenate([scaled, matches.astype(jnp.float32)]),
        weight_blocks,
        precision=grad_precision,
        preferred_element_type=jnp.float32,
    )

    row_peak = jnp.max(stats[:, 0], axis=0)
    row_total = jnp.sum(stats[:, 1] * jnp.exp(stats[:, 0] - row_peak), axis=0)
    target_logit = jnp.sum(stats[:, 2], axis=0)
    window_lse = row_peak + jnp.log(row_total)
    outside = rest_lse.reshape(tokens)
    ceiling = jnp.maximum(window_lse, outside)
    full_lse = ceiling + jnp.log(jnp.exp(window_lse - ceiling) + jnp.exp(outside - ceiling))
    local_scale = jnp.exp(local_peak - full_lse)
    partial_rows = both_rows[:, tokens:] - local_scale[None, :, None] * both_rows[:, :tokens]
    summed_rows = jnp.sum(exchanged(partial_rows, "vocab"), axis=0)

    positions = lax.iota(jnp.int32, seq_slots)
    live_tokens = (positions[None, None, :] < lengths[:, :, None]).astype(jnp.float32)
    token_logp = (target_logit - full_lse).reshape(pair_count, 2, seq_slots) * live_tokens
    sequence_logp = jnp.sum(token_logp, axis=2)
    margin = beta_scale * (
        sequence_logp[:, 0] - ref_logp[:, 0] - (sequence_logp[:, 1] - ref_logp[:, 1])
    )
    group_ids = lax.iota(jnp.int32, group_weight.shape[0])
    pair_weight = jnp.sum(
        jnp.where(group_map[:, None] == group_ids[None, :], group_weight[None, :], 0.0), axis=1
    )
    divisor = pair_count * jnp.sum(group_weight)
    local_loss = jnp.sum(pair_weight * jax.nn.softplus(-margin)) / divisor
    dpo_loss = summed_by_swaps(local_loss, "dp")
    coefficient = -beta_scale * pair_weight * jax.nn.sigmoid(-margin) / divisor
    sign_pair = jnp.array([1.0, -1.0], jnp.float32)
    token_grad = coefficient[:, None, None] * sign_pair[None, :, None] * live_tokens
    hidden_grad = token_grad[..., None] * summed_rows.reshape(hidden.shape)
    return (hidden_grad, dpo_loss)


def solution(mesh):
    return jax.shard_map(
        shards,
        mesh=mesh,
        in_specs=(
            P("dp", None, None, "vocab"),
            P(None, "vocab"),
            P("dp", None, None),
            P("dp", None),
            P("dp", None, None),
            P("dp", None),
            P("dp"),
            P(),
        ),
        out_specs=(P("dp", None, None, "vocab"), P()),
        check_vma=False,
    )
```

```python
import jax
import jax.numpy as jnp
from jax import lax
from jax.experimental import pallas as pl
from jax.experimental.pallas import tpu as pltpu
from jax.sharding import PartitionSpec as P

beta_scale = 0.05
both_axes = ("dp", "vocab")
side = 4


def line_groups(pairs, holders, first):
    groups = []
    for pair in range(pairs):
        along_x = (pair % 2 == 0) == first
        for line in range(side):
            places = [line * side + k if along_x else k * side + line for k in range(side)]
            groups.append([pair * holders + place for place in places])
    return groups


def plane_groups(pairs, holders):
    swapped = [(place % side) * side + place // side for place in range(holders)]
    return [
        [pair * holders + place for place in (range(holders) if pair % 2 == 0 else swapped)]
        for pair in range(pairs)
    ]


def near_groups(pairs, holders):
    return [
        [(block + k) * holders + place for k in range(2 * side)]
        for block in range(0, pairs, 2 * side)
        for place in range(holders)
    ]


def far_groups(pairs, holders):
    return [
        [(block + k) * holders + place for block in range(0, pairs, 2 * side)]
        for k in range(2 * side)
        for place in range(holders)
    ]


def exchanged(blocks, groups):
    return lax.all_to_all(
        blocks, both_axes, split_axis=0, concat_axis=0, axis_index_groups=groups, tiled=True
    )


def copies_from_line(shard, groups):
    return exchanged(jnp.broadcast_to(shard, (side, *shard.shape)), groups)


def split_parts(values):
    high = values.astype(jnp.bfloat16)
    low = (values - high.astype(jnp.float32)).astype(jnp.bfloat16)
    return high, low


def split_kernel(order_ref, block_ref, high_ref, low_ref):
    high_ref[...], low_ref[...] = split_parts(block_ref[...])


def split_weight(blocks, order):
    shape = (1, *blocks.shape[1:])
    part = jax.ShapeDtypeStruct(blocks.shape, jnp.bfloat16)
    return pl.pallas_call(
        split_kernel,
        out_shape=(part, part),
        grid_spec=pltpu.PrefetchScalarGridSpec(
            num_scalar_prefetch=1,
            grid=(blocks.shape[0],),
            in_specs=[pl.BlockSpec(shape, lambda k, order: (order[k], 0, 0))],
            out_specs=[pl.BlockSpec(shape, lambda k, order: (k, 0, 0))] * 2,
        ),
        compiler_params=pltpu.CompilerParams(vmem_limit_bytes=8 * 1024 * 1024),
        cost_estimate=pl.CostEstimate(
            flops=4_000_000_000, bytes_accessed=2 * blocks.size * 4, transcendentals=0
        ),
    )(order, blocks)


def product(both, high, low, dims):
    rows = both.shape[0] // 2
    wide = lax.dot_general(both, high, dims, preferred_element_type=jnp.float32)
    narrow = lax.dot_general(both[:rows], low, dims, preferred_element_type=jnp.float32)
    return wide[:rows] + (wide[rows:] + narrow)


def logits_kernel(states_ref, high_ref, low_ref, out_ref):
    total = None
    for k in range(states_ref.shape[0]):
        both = jnp.concatenate(split_parts(states_ref[k]), axis=0)
        term = product(both, high_ref[k], low_ref[k], (((1,), (0,)), ((), ())))
        total = term if total is None else total + term

    @pl.when(pl.program_id(0) == 0)
    def _():
        out_ref[...] = total

    @pl.when(pl.program_id(0) != 0)
    def _():
        out_ref[...] += total


def rows_kernel(grad_ref, high_ref, low_ref, out_ref):
    both = jnp.concatenate(split_parts(grad_ref[...]), axis=0)
    for k in range(out_ref.shape[0]):
        out_ref[k] = product(both, high_ref[k], low_ref[k], (((1,), (1,)), ((), ())))


def logits_of(states, high, low):
    holders, tokens, width = states.shape
    columns = high.shape[2]
    weight_spec = pl.BlockSpec((side, width, columns), lambda k: (k, 0, 0))
    return pl.pallas_call(
        logits_kernel,
        out_shape=jax.ShapeDtypeStruct((tokens, columns), jnp.float32),
        grid=(holders // side,),
        in_specs=[pl.BlockSpec((side, tokens, width), lambda k: (k, 0, 0)), weight_spec, weight_spec],
        out_specs=pl.BlockSpec((tokens, columns), lambda k: (0, 0)),
        compiler_params=pltpu.CompilerParams(vmem_limit_bytes=16 * 1024 * 1024),
        cost_estimate=pl.CostEstimate(
            flops=6 * tokens * width * holders * columns,
            bytes_accessed=4 * (states.size + high.size),
            transcendentals=0,
        ),
    )(states, high, low)


def rows_of(row_grad, high, low):
    tokens, columns = row_grad.shape
    holders, width, _ = high.shape
    weight_spec = pl.BlockSpec((side, width, columns), lambda k: (k, 0, 0))
    return pl.pallas_call(
        rows_kernel,
        out_shape=jax.ShapeDtypeStruct((holders, tokens, width), jnp.float32),
        grid=(holders // side,),
        in_specs=[pl.BlockSpec((tokens, columns), lambda k: (0, 0)), weight_spec, weight_spec],
        out_specs=pl.BlockSpec((side, tokens, width), lambda k: (k, 0, 0)),
        compiler_params=pltpu.CompilerParams(vmem_limit_bytes=16 * 1024 * 1024),
        cost_estimate=pl.CostEstimate(
            flops=6 * tokens * width * holders * columns,
            bytes_accessed=4 * (holders * tokens * width + high.size),
            transcendentals=0,
        ),
    )(row_grad, high, low)


def shards(hidden, head_weight, targets, lengths, rest_lse, ref_logp, group_map, group_weight):
    pair_count, _, seq_slots, local_width = hidden.shape
    column_count = head_weight.shape[1]
    pairs, holders = lax.axis_size("dp"), lax.axis_size("vocab")
    first_lines = line_groups(pairs, holders, True)
    second_lines = line_groups(pairs, holders, False)
    tokens = pair_count * 2 * seq_slots

    near = copies_from_line(hidden.reshape(tokens, local_width), first_lines)
    states = copies_from_line(near, second_lines).reshape(holders, tokens, local_width)

    places = lax.iota(jnp.int32, holders)
    swapped = (places % side) * side + places // side
    order = jnp.where(lax.axis_index("dp") % 2 == 0, places, swapped)
    high, low = split_weight(head_weight.reshape(holders, local_width, column_count), order)
    column_ids = lax.axis_index("vocab") * column_count + lax.iota(jnp.int32, column_count)
    matches = targets.reshape(tokens)[:, None] == column_ids[None, :]

    logits = logits_of(states, high, low)
    local_peak = jnp.max(logits, axis=1)
    scaled = jnp.exp(logits - local_peak[:, None])
    local_total = jnp.sum(scaled, axis=1)
    local_target = jnp.sum(jnp.where(matches, logits, 0.0), axis=1)
    local_stats = jnp.stack([local_peak, local_total, local_target])
    stats = lax.all_to_all(
        jnp.broadcast_to(local_stats, (holders, *local_stats.shape)), "vocab", 0, 0, tiled=True
    )

    row_peak = jnp.max(stats[:, 0], axis=0)
    row_total = jnp.sum(stats[:, 1] * jnp.exp(stats[:, 0] - row_peak), axis=0)
    target_logit = jnp.sum(stats[:, 2], axis=0)
    window_lse = row_peak + jnp.log(row_total)
    outside = rest_lse.reshape(tokens)
    ceiling = jnp.maximum(window_lse, outside)
    full_lse = ceiling + jnp.log(jnp.exp(window_lse - ceiling) + jnp.exp(outside - ceiling))
    local_scale = jnp.exp(local_peak - full_lse)
    row_grad = matches.astype(jnp.float32) - local_scale[:, None] * scaled
    partial_rows = rows_of(row_grad, high, low)
    summed_rows = jnp.sum(exchanged(partial_rows, plane_groups(pairs, holders)), axis=0)

    positions = lax.iota(jnp.int32, seq_slots)
    live_tokens = (positions[None, None, :] < lengths[:, :, None]).astype(jnp.float32)
    token_logp = (target_logit - full_lse).reshape(pair_count, 2, seq_slots) * live_tokens
    sequence_logp = jnp.sum(token_logp, axis=2)
    margin = beta_scale * (
        sequence_logp[:, 0] - ref_logp[:, 0] - (sequence_logp[:, 1] - ref_logp[:, 1])
    )
    group_ids = lax.iota(jnp.int32, group_weight.shape[0])
    pair_weight = jnp.sum(
        jnp.where(group_map[:, None] == group_ids[None, :], group_weight[None, :], 0.0), axis=1
    )
    divisor = pair_count * jnp.sum(group_weight)
    pair_losses = pair_weight * jax.nn.softplus(-margin)
    loss_row = jnp.broadcast_to(jnp.sum(pair_losses, keepdims=True)[None], (1, 128))
    loss_row = lax.psum(loss_row, both_axes, axis_index_groups=near_groups(pairs, holders))
    loss_row = lax.psum(loss_row, both_axes, axis_index_groups=far_groups(pairs, holders))
    dpo_loss = loss_row[0, 0] / divisor
    coefficient = -beta_scale * pair_weight * jax.nn.sigmoid(-margin) / divisor
    sign_pair = jnp.array([1.0, -1.0], jnp.float32)
    token_grad = coefficient[:, None, None] * sign_pair[None, :, None] * live_tokens
    hidden_grad = token_grad[..., None] * summed_rows.reshape(hidden.shape)
    return (hidden_grad, dpo_loss)


def solution(mesh):
    return jax.shard_map(
        shards,
        mesh=mesh,
        in_specs=(
            P("dp", None, None, "vocab"),
            P(None, "vocab"),
            P("dp", None, None),
            P("dp", None),
            P("dp", None, None),
            P("dp", None),
            P("dp"),
            P(),
        ),
        out_specs=(P("dp", None, None, "vocab"), P()),
        check_vma=False,
    )
```

```python
import jax
import jax.numpy as jnp
from jax import lax
from jax.experimental import pallas as pl
from jax.experimental.pallas import tpu as pltpu
from jax.sharding import PartitionSpec as P

beta_scale = 0.05
both_axes = ("dp", "vocab")
near_members = 8
stat_rows = 8
vmem_grant = 24 * 1024 * 1024


def near_groups(pairs, holders):
    return [
        [(block + k) * holders + place for k in range(near_members)]
        for block in range(0, pairs, near_members)
        for place in range(holders)
    ]


def far_groups(pairs, holders):
    return [
        [(block + k) * holders + place for block in range(0, pairs, near_members)]
        for k in range(near_members)
        for place in range(holders)
    ]


def split_parts(values):
    high = values.astype(jnp.bfloat16)
    low = (values - high.astype(jnp.float32)).astype(jnp.bfloat16)
    return high, low


def stacked_parts(values):
    return jnp.concatenate(split_parts(values), axis=0)


def product(both, weight, weight_dim):
    rows = both.shape[0] // 2
    high, low = split_parts(weight)
    dims = (((1,), (weight_dim,)), ((), ()))
    wide = lax.dot_general(both, high, dims, preferred_element_type=jnp.float32)
    narrow = lax.dot_general(both[:rows], low, dims, preferred_element_type=jnp.float32)
    return wide[:rows] + (wide[rows:] + narrow)


def column_matches(target_row, base, columns):
    ids = base + lax.broadcasted_iota(jnp.int32, (columns, target_row.shape[1]), 0)
    return ids == target_row


def copies_kernel(shard_ref, base_ref, target_ref, outside_ref, out_ref):
    shard = shard_ref[...]
    for k in range(out_ref.shape[0]):
        out_ref[k] = shard


def copies_for_all(shard, holders, base, target_row, outside_row):
    return pl.pallas_call(
        copies_kernel,
        out_shape=jax.ShapeDtypeStruct((holders, *shard.shape), shard.dtype),
        in_specs=[pl.BlockSpec(memory_space=pltpu.VMEM), pl.BlockSpec(memory_space=pltpu.SMEM)]
        + [pl.BlockSpec(memory_space=pltpu.VMEM)] * 2,
        out_specs=pl.BlockSpec(memory_space=pltpu.VMEM),
        compiler_params=pltpu.CompilerParams(vmem_limit_bytes=vmem_grant),
        name="state_copies",
    )(shard, base, target_row, outside_row)


def logits_kernel(base_ref, states_ref, target_ref, weight_ref, scaled_ref, own_ref, stats_ref):
    total = product(stacked_parts(states_ref[0]), weight_ref[0], 0)
    for k in range(1, states_ref.shape[0]):
        total += product(stacked_parts(states_ref[k]), weight_ref[k], 0)
    logits = total.T
    peak = jnp.max(logits, axis=0, keepdims=True)
    scaled = jnp.exp(logits - peak)
    scaled_ref[...] = scaled
    matches = column_matches(target_ref[...], base_ref[0], logits.shape[0])
    exponentials = jnp.sum(scaled, axis=0, keepdims=True)
    target = jnp.sum(jnp.where(matches, logits, 0.0), axis=0, keepdims=True)
    row = lax.broadcasted_iota(jnp.int32, own_ref.shape, 0)
    stats = jnp.where(row == 0, peak, jnp.where(row == 1, exponentials, target))
    own_ref[...] = stats
    for k in range(stats_ref.shape[0]):
        stats_ref[k] = stats


def local_logits(base, states, target_row, weight_blocks):
    holders, tokens, _ = states.shape
    columns = weight_blocks.shape[2]
    return pl.pallas_call(
        logits_kernel,
        out_shape=(
            jax.ShapeDtypeStruct((columns, tokens), jnp.float32),
            jax.ShapeDtypeStruct((stat_rows, tokens), jnp.float32),
            jax.ShapeDtypeStruct((holders, stat_rows, tokens), jnp.float32),
        ),
        in_specs=[
            pl.BlockSpec(memory_space=pltpu.SMEM),
            pl.BlockSpec(memory_space=pltpu.VMEM),
            pl.BlockSpec(memory_space=pltpu.VMEM),
            pl.BlockSpec(memory_space=pltpu.VMEM),
        ],
        out_specs=(pl.BlockSpec(memory_space=pltpu.VMEM),) * 3,
        compiler_params=pltpu.CompilerParams(vmem_limit_bytes=vmem_grant),
        cost_estimate=pl.CostEstimate(
            flops=6 * states.size * columns,
            bytes_accessed=4 * (states.size + weight_blocks.size),
            transcendentals=tokens * columns,
        ),
        name="local_logits",
    )(base, states, target_row, weight_blocks)


def softplus(values):
    small = jnp.exp(-jnp.abs(values))
    shifted = 1.0 + small
    gap = shifted - 1.0
    safe = jnp.where(gap == 0.0, 1.0, gap)
    log_shifted = jnp.where(gap == 0.0, small, jnp.log(shifted) * (small / safe))
    return jnp.maximum(values, 0.0) + log_shifted


def rows_kernel(
    base_ref,
    lengths_ref,
    ref_logp_ref,
    group_map_ref,
    weight_of_ref,
    stats_ref,
    own_ref,
    scaled_ref,
    target_ref,
    outside_ref,
    weight_ref,
    rows_ref,
    loss_ref,
    made_ref,
    sems,
):
    pair_count, seq_slots = lengths_ref.shape[0], target_ref.shape[1] // lengths_ref.size
    stats = stats_ref[...]
    peaks, totals, targets = (stats[:, k : k + 1] for k in range(3))
    row_peak = jnp.max(peaks, axis=0)
    row_total = jnp.sum(totals * jnp.exp(peaks - row_peak[None]), axis=0)
    target_logit = jnp.sum(targets, axis=0)
    window_lse = row_peak + jnp.log(row_total)
    outside = outside_ref[...]
    ceiling = jnp.maximum(window_lse, outside)
    full_lse = ceiling + jnp.log(jnp.exp(window_lse - ceiling) + jnp.exp(outside - ceiling))

    token = lax.broadcasted_iota(jnp.int32, outside.shape, 1)
    slot, sequence = token % seq_slots, token // seq_slots
    divisor = 0.0
    for k in range(weight_of_ref.shape[0]):
        divisor += weight_of_ref[k]
    divisor = pair_count * divisor
    token_grad = jnp.zeros(outside.shape, jnp.float32)
    loss = jnp.zeros((1, 1), jnp.float32)
    for pair in range(pair_count):
        scores, masks = [], []
        for one in range(2):
            live = (sequence == 2 * pair + one) & (slot < lengths_ref[pair, one])
            kept = jnp.where(live, target_logit - full_lse, 0.0)
            scores.append(jnp.sum(kept, axis=1, keepdims=True) - ref_logp_ref[pair, one])
            masks.append(live)
        margin = beta_scale * (scores[0] - scores[1])
        pair_weight = weight_of_ref[group_map_ref[pair]]
        loss += pair_weight * softplus(-margin) / divisor
        coefficient = -beta_scale * pair_weight / (1.0 + jnp.exp(margin)) / divisor
        token_grad += jnp.where(masks[0], coefficient, 0.0)
        token_grad -= jnp.where(masks[1], coefficient, 0.0)
    loss_ref[...] = jnp.broadcast_to(loss, loss_ref.shape)

    scale = jnp.exp(own_ref[0:1] - full_lse)
    matches = column_matches(target_ref[...], base_ref[0], scaled_ref.shape[0])
    grad = token_grad * (matches.astype(jnp.float32) - scale * scaled_ref[...])
    both = stacked_parts(grad.T)
    sent = []
    for k in range(made_ref.shape[0]):
        made_ref[k] = product(both, weight_ref[k], 1)
        sent.append(pltpu.make_async_copy(made_ref.at[k], rows_ref.at[k], sems.at[k]))
        sent[k].start()
    for copy in sent:
        copy.wait()


def gradient_rows(scalars, arrays, weight_blocks, tokens):
    holders, width, columns = weight_blocks.shape
    rows_shape = (holders, tokens, width)
    return pl.pallas_call(
        rows_kernel,
        out_shape=(
            pltpu.HBM(rows_shape, jnp.float32),
            jax.ShapeDtypeStruct((1, tokens), jnp.float32),
        ),
        in_specs=[pl.BlockSpec(memory_space=pltpu.SMEM)] * len(scalars)
        + [pl.BlockSpec(memory_space=pltpu.VMEM)] * (len(arrays) + 1),
        out_specs=(pl.BlockSpec(memory_space=pltpu.HBM), pl.BlockSpec(memory_space=pltpu.VMEM)),
        scratch_shapes=[pltpu.VMEM(rows_shape, jnp.float32), pltpu.SemaphoreType.DMA((holders,))],
        compiler_params=pltpu.CompilerParams(vmem_limit_bytes=vmem_grant),
        cost_estimate=pl.CostEstimate(
            flops=6 * tokens * weight_blocks.size,
            bytes_accessed=4 * (holders * tokens * width + weight_blocks.size),
            transcendentals=tokens * holders,
        ),
        name="gradient_rows",
    )(*scalars, *arrays, weight_blocks)


def shards(hidden, head_weight, targets, lengths, rest_lse, ref_logp, group_map, group_weight):
    pair_count, _, seq_slots, local_width = hidden.shape
    column_count = head_weight.shape[1]
    pairs, holders = lax.axis_size("dp"), lax.axis_size("vocab")
    tokens = pair_count * 2 * seq_slots
    weight_blocks = head_weight.reshape(holders, local_width, column_count)
    base = (lax.axis_index("vocab") * column_count).astype(jnp.int32).reshape(1)
    target_row = targets.reshape(1, tokens)
    outside_row = rest_lse.reshape(1, tokens)

    state_copies = copies_for_all(
        hidden.reshape(tokens, local_width), holders, base, target_row, outside_row
    )
    states = lax.all_to_all(state_copies, "vocab", 0, 0, tiled=True)
    scaled, own_stats, stat_copies = local_logits(base, states, target_row, weight_blocks)
    stats = lax.all_to_all(stat_copies, "vocab", 0, 0, tiled=True)
    partial_rows, loss_row = gradient_rows(
        (base, lengths, ref_logp, group_map, group_weight),
        (stats, own_stats, scaled, target_row, outside_row),
        weight_blocks,
        tokens,
    )
    summed_rows = jnp.sum(lax.all_to_all(partial_rows, "vocab", 0, 0, tiled=True), axis=0)
    loss_row = lax.psum(loss_row, both_axes, axis_index_groups=near_groups(pairs, holders))
    loss_row = lax.psum(loss_row, both_axes, axis_index_groups=far_groups(pairs, holders))
    return (summed_rows.reshape(hidden.shape), loss_row[0, 0])


def solution(mesh):
    return jax.shard_map(
        shards,
        mesh=mesh,
        in_specs=(
            P("dp", None, None, "vocab"),
            P(None, "vocab"),
            P("dp", None, None),
            P("dp", None),
            P("dp", None, None),
            P("dp", None),
            P("dp"),
            P(),
        ),
        out_specs=(P("dp", None, None, "vocab"), P()),
        check_vma=False,
    )
```

```python
import functools

import jax
import jax.numpy as jnp
from jax import lax
from jax.experimental import pallas as pl
from jax.experimental.pallas import tpu as pltpu
from jax.sharding import PartitionSpec as P

beta_scale = 0.05
both_axes = ("dp", "vocab")
cores = 2
near_chips = 4
stat_rows = 8
vmem_grant = 24 * 1024 * 1024


def chip_plane_groups(pairs, holders):
    return [
        [pair * holders + place for pair in (first, first + 1) for place in range(holders)]
        for first in range(0, pairs, cores)
    ]


def near_groups(pairs, holders):
    block = cores * near_chips
    return [
        [(start + k) * holders + place for k in range(0, block, cores)]
        for first in range(0, pairs, block)
        for start in range(first, first + cores)
        for place in range(holders)
    ]


def far_groups(pairs, holders):
    block = cores * near_chips
    return [
        [(first + k) * holders + place for first in range(0, pairs, block)]
        for k in range(block)
        for place in range(holders)
    ]


def split_parts(values):
    high = values.astype(jnp.bfloat16)
    low = (values - high.astype(jnp.float32)).astype(jnp.bfloat16)
    return high, low


def stacked_parts(values):
    return jnp.concatenate(split_parts(values), axis=0)


def product(both, weight, weight_dim):
    rows = both.shape[0] // 2
    high, low = split_parts(weight)
    dims = (((1,), (weight_dim,)), ((), ()))
    wide = lax.dot_general(both, high, dims, preferred_element_type=jnp.float32)
    narrow = lax.dot_general(both[:rows], low, dims, preferred_element_type=jnp.float32)
    return wide[:rows] + (wide[rows:] + narrow)


def column_matches(target_row, base, columns):
    ids = base + lax.broadcasted_iota(jnp.int32, (columns, target_row.shape[1]), 0)
    return ids == target_row


def copies_kernel(shard_ref, out_ref):
    shard = shard_ref[...]
    for k in range(out_ref.shape[0]):
        out_ref[k] = shard


def copies_for_all(shard, holders):
    return pl.pallas_call(
        copies_kernel,
        out_shape=jax.ShapeDtypeStruct((holders, *shard.shape), shard.dtype),
        in_specs=[pl.BlockSpec(memory_space=pltpu.VMEM)],
        out_specs=pl.BlockSpec(memory_space=pltpu.VMEM),
        compiler_params=pltpu.CompilerParams(vmem_limit_bytes=vmem_grant),
        name="state_copies",
    )(shard)


def token_row(values_ref):
    pairs, ones, _ = values_ref.shape
    pieces = [values_ref[pair, one : one + 1] for pair in range(pairs) for one in range(ones)]
    return jnp.concatenate(pieces, axis=1)


def logits_kernel(
    lengths_ref,
    ref_logp_ref,
    group_map_ref,
    weight_of_ref,
    targets_ref,
    rest_lse_ref,
    states_ref,
    weight_ref,
    scaled_ref,
    matches_ref,
    own_ref,
    stats_ref,
):
    pair_count, _, seq_slots = targets_ref.shape
    target_row = token_row(targets_ref)
    token = lax.broadcasted_iota(jnp.int32, target_row.shape, 1)
    slot, sequence = token % seq_slots, token // seq_slots
    divisor = 0.0
    for k in range(weight_of_ref.shape[0]):
        divisor += weight_of_ref[k]
    divisor = pair_count * divisor
    live = jnp.zeros(target_row.shape, jnp.float32)
    prior = jnp.zeros(target_row.shape, jnp.float32)
    share = jnp.zeros(target_row.shape, jnp.float32)
    for pair in range(pair_count):
        pair_share = weight_of_ref[group_map_ref[pair]]
        for one in range(2):
            here = sequence == 2 * pair + one
            live = jnp.where(here & (slot < lengths_ref[pair, one]), 1.0, live)
            prior = jnp.where(here, ref_logp_ref[pair, one], prior)
            share = jnp.where(here, pair_share, share)
    share = share / divisor

    total = product(stacked_parts(states_ref[0]), weight_ref[0], 0)
    for k in range(1, states_ref.shape[0]):
        total += product(stacked_parts(states_ref[k]), weight_ref[k], 0)
    logits = total.T
    peak = jnp.max(logits, axis=0, keepdims=True)
    scaled = jnp.exp(logits - peak)
    scaled_ref[...] = scaled
    ids = lax.axis_index("vocab") * logits.shape[0] + lax.broadcasted_iota(jnp.int32, logits.shape, 0)
    matches = ids == target_row
    matches_ref[...] = matches.astype(jnp.float32)
    exponentials = jnp.sum(scaled, axis=0, keepdims=True)
    target = jnp.sum(jnp.where(matches, logits, 0.0), axis=0, keepdims=True)
    row = lax.broadcasted_iota(jnp.int32, own_ref.shape, 0)
    stats = jnp.zeros(own_ref.shape, jnp.float32)
    for k, values in enumerate((peak, exponentials, target, token_row(rest_lse_ref), live, prior, share)):
        stats = jnp.where(row == k, values, stats)
    own_ref[...] = stats
    for k in range(stats_ref.shape[0]):
        stats_ref[k] = stats


def local_logits(scalars, targets, rest_lse, states, weight_blocks):
    holders, tokens, _ = states.shape
    columns = weight_blocks.shape[2]
    in_vmem = pl.BlockSpec(memory_space=pltpu.VMEM)
    return pl.pallas_call(
        logits_kernel,
        out_shape=(
            jax.ShapeDtypeStruct((columns, tokens), jnp.float32),
            jax.ShapeDtypeStruct((columns, tokens), jnp.float32),
            jax.ShapeDtypeStruct((stat_rows, tokens), jnp.float32),
            jax.ShapeDtypeStruct((cores * holders, stat_rows, tokens), jnp.float32),
        ),
        in_specs=[pl.BlockSpec(memory_space=pltpu.SMEM)] * len(scalars) + [in_vmem] * 4,
        out_specs=(in_vmem,) * 4,
        compiler_params=pltpu.CompilerParams(vmem_limit_bytes=vmem_grant),
        cost_estimate=pl.CostEstimate(
            flops=6 * states.size * columns,
            bytes_accessed=4 * (states.size + weight_blocks.size),
            transcendentals=tokens * columns,
        ),
        name="local_logits",
    )(*scalars, targets, rest_lse, states, weight_blocks)


def softplus(values):
    small = jnp.exp(-jnp.abs(values))
    shifted = 1.0 + small
    gap = shifted - 1.0
    safe = jnp.where(gap == 0.0, 1.0, gap)
    log_shifted = jnp.where(gap == 0.0, small, jnp.log(shifted) * (small / safe))
    return jnp.maximum(values, 0.0) + log_shifted


def joined(stats):
    peaks, totals, targets = (stats[:, k : k + 1] for k in range(3))
    row_peak = jnp.max(peaks, axis=0)
    row_total = jnp.sum(totals * jnp.exp(peaks - row_peak[None]), axis=0)
    window_lse = row_peak + jnp.log(row_total)
    outside = stats[0, 3:4]
    ceiling = jnp.maximum(window_lse, outside)
    full_lse = ceiling + jnp.log(jnp.exp(window_lse - ceiling) + jnp.exp(outside - ceiling))
    return full_lse, jnp.sum(targets, axis=0)


def preference(full_lse, target_logit, live, prior, share, pair_count):
    tokens = live.shape[1]
    sequence = lax.broadcasted_iota(jnp.int32, live.shape, 1) // (tokens // (2 * pair_count))
    token_logp = live * (target_logit - full_lse)
    token_grad = jnp.zeros(live.shape, jnp.float32)
    loss = jnp.zeros((1, 1), jnp.float32)

    def of_sequence(values, here):
        return jnp.sum(jnp.where(here, values, 0.0), axis=1, keepdims=True)

    def first_of(values, here):
        return jnp.max(jnp.where(here, values, -jnp.inf), axis=1, keepdims=True)

    for pair in range(pair_count):
        chosen, rejected = (sequence == 2 * pair + one for one in range(2))
        margin = beta_scale * (
            (of_sequence(token_logp, chosen) - first_of(prior, chosen))
            - (of_sequence(token_logp, rejected) - first_of(prior, rejected))
        )
        pair_share = first_of(share, chosen)
        loss += pair_share * softplus(-margin)
        coefficient = -beta_scale * pair_share / (1.0 + jnp.exp(margin))
        token_grad += jnp.where(chosen, coefficient, 0.0) - jnp.where(rejected, coefficient, 0.0)
    return loss, live * token_grad


def rows_kernel(
    pair_count, stats_ref, own_ref, scaled_ref, matches_ref, weight_ref, rows_ref, loss_ref, grads_ref, made_ref, sems
):
    holders = weight_ref.shape[0]
    own_core = lax.axis_index("dp") % cores
    mine = pl.ds(pl.multiple_of(own_core * holders, holders), holders)
    full_lse, _ = joined(stats_ref[mine])
    scale = jnp.exp(own_ref[0:1] - full_lse)
    both = stacked_parts((matches_ref[...] - scale * scaled_ref[...]).T)
    sent = []
    for k in range(holders):
        made_ref[k] = product(both, weight_ref[k], 1)
        sent.append(pltpu.make_async_copy(made_ref.at[k], rows_ref.at[k], sems.at[k]))
        sent[k].start()
    loss = jnp.zeros((1, 1), jnp.float32)
    token_grad = jnp.zeros(loss_ref.shape, jnp.float32)
    for core in range(cores):
        stats = stats_ref[pl.ds(core * holders, holders)]
        given = (stats[0, k : k + 1] for k in range(4, 7))
        core_loss, core_grad = preference(*joined(stats), *given, pair_count)
        loss += core_loss
        token_grad = jnp.where(own_core == core, core_grad, token_grad)
    loss_ref[...] = jnp.broadcast_to(loss, loss_ref.shape)
    grads_ref[...] = jnp.broadcast_to(token_grad, grads_ref.shape[::-1]).T
    for copy in sent:
        copy.wait()


def gradient_rows(pair_count, stats, own, scaled, matches, weight_blocks):
    holders, width, columns = weight_blocks.shape
    tokens = own.shape[1]
    rows_shape = (holders, tokens, width)
    in_vmem = pl.BlockSpec(memory_space=pltpu.VMEM)
    return pl.pallas_call(
        functools.partial(rows_kernel, pair_count),
        out_shape=(
            pltpu.HBM(rows_shape, jnp.float32),
            jax.ShapeDtypeStruct((1, tokens), jnp.float32),
            jax.ShapeDtypeStruct((tokens, width), jnp.float32),
        ),
        in_specs=[in_vmem] * 5,
        out_specs=(pl.BlockSpec(memory_space=pltpu.HBM), in_vmem, in_vmem),
        scratch_shapes=[pltpu.VMEM(rows_shape, jnp.float32), pltpu.SemaphoreType.DMA((holders,))],
        compiler_params=pltpu.CompilerParams(vmem_limit_bytes=vmem_grant),
        cost_estimate=pl.CostEstimate(
            flops=6 * tokens * weight_blocks.size,
            bytes_accessed=4 * (holders * tokens * width + weight_blocks.size),
            transcendentals=tokens * holders,
        ),
        name="gradient_rows",
    )(stats, own, scaled, matches, weight_blocks)


def shards(hidden, head_weight, targets, lengths, rest_lse, ref_logp, group_map, group_weight):
    pair_count, _, seq_slots, local_width = hidden.shape
    pairs, holders = lax.axis_size("dp"), lax.axis_size("vocab")
    tokens = pair_count * 2 * seq_slots
    weight_blocks = head_weight.reshape(holders, local_width, -1)

    state_copies = copies_for_all(hidden.reshape(tokens, local_width), holders)
    states = lax.all_to_all(state_copies, "vocab", 0, 0, tiled=True)
    scaled, matches, own_stats, stat_copies = local_logits(
        (lengths, ref_logp, group_map, group_weight), targets, rest_lse, states, weight_blocks
    )
    stats = lax.all_to_all(
        stat_copies, both_axes, 0, 0, axis_index_groups=chip_plane_groups(pairs, holders), tiled=True
    )
    partial_rows, loss_row, token_grads = gradient_rows(
        pair_count, stats, own_stats, scaled, matches, weight_blocks
    )
    summed_rows = jnp.sum(lax.all_to_all(partial_rows, "vocab", 0, 0, tiled=True), axis=0)
    loss_row = lax.psum(loss_row, both_axes, axis_index_groups=near_groups(pairs, holders))
    loss_row = lax.psum(loss_row, both_axes, axis_index_groups=far_groups(pairs, holders))
    return ((token_grads * summed_rows).reshape(hidden.shape), loss_row[0, 0])


def solution(mesh):
    return jax.shard_map(
        shards,
        mesh=mesh,
        in_specs=(
            P("dp", None, None, "vocab"),
            P(None, "vocab"),
            P("dp", None, None),
            P("dp", None),
            P("dp", None, None),
            P("dp", None),
            P("dp"),
            P(),
        ),
        out_specs=(P("dp", None, None, "vocab"), P()),
        check_vma=False,
    )
```

```python
import functools

import jax
import jax.numpy as jnp
from jax import lax
from jax.experimental import pallas as pl
from jax.experimental.pallas import tpu as pltpu
from jax.sharding import PartitionSpec as P

beta_scale = 0.05
both_axes = ("dp", "vocab")
cores = 2
side = 4
near_chips = 4
stat_rows = 8
vmem_grant = 24 * 1024 * 1024


def line_groups(pairs, holders, first):
    groups = []
    for pair in range(pairs):
        along_x = (pair % cores == 0) == first
        for line in range(side):
            places = [line * side + k if along_x else k * side + line for k in range(side)]
            groups.append([pair * holders + place for place in places])
    return groups


def chip_plane_groups(pairs, holders):
    return [
        [pair * holders + place for pair in (first, first + 1) for place in range(holders)]
        for first in range(0, pairs, cores)
    ]


def near_groups(pairs, holders):
    block = cores * near_chips
    return [
        [(start + k) * holders + place for k in range(0, block, cores)]
        for first in range(0, pairs, block)
        for start in range(first, first + cores)
        for place in range(holders)
    ]


def far_groups(pairs, holders):
    block = cores * near_chips
    return [
        [(first + k) * holders + place for first in range(0, pairs, block)]
        for k in range(block)
        for place in range(holders)
    ]


def split_parts(values):
    high = values.astype(jnp.bfloat16)
    low = (values - high.astype(jnp.float32)).astype(jnp.bfloat16)
    return high, low


def stacked_parts(values):
    return jnp.concatenate(split_parts(values), axis=0)


def product(both, weight, weight_dim):
    rows = both.shape[0] // 2
    high, low = split_parts(weight)
    dims = (((1,), (weight_dim,)), ((), ()))
    wide = lax.dot_general(both, high, dims, preferred_element_type=jnp.float32)
    narrow = lax.dot_general(both[:rows], low, dims, preferred_element_type=jnp.float32)
    return wide[:rows] + (wide[rows:] + narrow)


def column_matches(target_row, base, columns):
    ids = base + lax.broadcasted_iota(jnp.int32, (columns, target_row.shape[1]), 0)
    return ids == target_row


def holder_of(block, own_core):
    return jnp.where(own_core == 0, block, (block % side) * side + block // side)


def copies_kernel(shard_ref, out_ref):
    shard = shard_ref[...]
    for k in range(out_ref.shape[0]):
        out_ref[k] = shard


def copies_for_all(shard, holders):
    return pl.pallas_call(
        copies_kernel,
        out_shape=jax.ShapeDtypeStruct((holders, *shard.shape), shard.dtype),
        in_specs=[pl.BlockSpec(memory_space=pltpu.VMEM)],
        out_specs=pl.BlockSpec(memory_space=pltpu.VMEM),
        compiler_params=pltpu.CompilerParams(vmem_limit_bytes=vmem_grant),
        name="state_copies",
    )(shard)


def token_row(values_ref):
    pairs, ones, _ = values_ref.shape
    pieces = [values_ref[pair, one : one + 1] for pair in range(pairs) for one in range(ones)]
    return jnp.concatenate(pieces, axis=1)


def logits_kernel(
    lengths_ref,
    ref_logp_ref,
    group_map_ref,
    weight_of_ref,
    targets_ref,
    rest_lse_ref,
    states_ref,
    weight_ref,
    scaled_ref,
    matches_ref,
    own_ref,
    stats_ref,
):
    pair_count, _, seq_slots = targets_ref.shape
    target_row = token_row(targets_ref)
    token = lax.broadcasted_iota(jnp.int32, target_row.shape, 1)
    slot, sequence = token % seq_slots, token // seq_slots
    divisor = 0.0
    for k in range(weight_of_ref.shape[0]):
        divisor += weight_of_ref[k]
    divisor = pair_count * divisor
    live = jnp.zeros(target_row.shape, jnp.float32)
    prior = jnp.zeros(target_row.shape, jnp.float32)
    share = jnp.zeros(target_row.shape, jnp.float32)
    for pair in range(pair_count):
        pair_share = weight_of_ref[group_map_ref[pair]]
        for one in range(2):
            here = sequence == 2 * pair + one
            live = jnp.where(here & (slot < lengths_ref[pair, one]), 1.0, live)
            prior = jnp.where(here, ref_logp_ref[pair, one], prior)
            share = jnp.where(here, pair_share, share)
    share = share / divisor

    own_core = lax.axis_index("dp") % cores
    total = product(stacked_parts(states_ref[0]), weight_ref[0], 0)
    for k in range(1, states_ref.shape[0]):
        total += product(stacked_parts(states_ref[k]), weight_ref[holder_of(k, own_core)], 0)
    logits = total.T
    peak = jnp.max(logits, axis=0, keepdims=True)
    scaled = jnp.exp(logits - peak)
    scaled_ref[...] = scaled
    ids = lax.axis_index("vocab") * logits.shape[0] + lax.broadcasted_iota(jnp.int32, logits.shape, 0)
    matches = ids == target_row
    matches_ref[...] = matches.astype(jnp.float32)
    exponentials = jnp.sum(scaled, axis=0, keepdims=True)
    target = jnp.sum(jnp.where(matches, logits, 0.0), axis=0, keepdims=True)
    row = lax.broadcasted_iota(jnp.int32, own_ref.shape, 0)
    stats = jnp.zeros(own_ref.shape, jnp.float32)
    for k, values in enumerate((peak, exponentials, target, token_row(rest_lse_ref), live, prior, share)):
        stats = jnp.where(row == k, values, stats)
    own_ref[...] = stats
    for k in range(stats_ref.shape[0]):
        stats_ref[k] = stats


def local_logits(scalars, targets, rest_lse, states, weight_blocks):
    holders, tokens, _ = states.shape
    columns = weight_blocks.shape[2]
    in_vmem = pl.BlockSpec(memory_space=pltpu.VMEM)
    return pl.pallas_call(
        logits_kernel,
        out_shape=(
            jax.ShapeDtypeStruct((columns, tokens), jnp.float32),
            jax.ShapeDtypeStruct((columns, tokens), jnp.float32),
            jax.ShapeDtypeStruct((stat_rows, tokens), jnp.float32),
            jax.ShapeDtypeStruct((cores * holders, stat_rows, tokens), jnp.float32),
        ),
        in_specs=[pl.BlockSpec(memory_space=pltpu.SMEM)] * len(scalars) + [in_vmem] * 4,
        out_specs=(in_vmem,) * 4,
        compiler_params=pltpu.CompilerParams(vmem_limit_bytes=vmem_grant),
        cost_estimate=pl.CostEstimate(
            flops=6 * states.size * columns,
            bytes_accessed=4 * (states.size + weight_blocks.size),
            transcendentals=tokens * columns,
        ),
        name="local_logits",
    )(*scalars, targets, rest_lse, states, weight_blocks)


def softplus(values):
    small = jnp.exp(-jnp.abs(values))
    shifted = 1.0 + small
    gap = shifted - 1.0
    safe = jnp.where(gap == 0.0, 1.0, gap)
    log_shifted = jnp.where(gap == 0.0, small, jnp.log(shifted) * (small / safe))
    return jnp.maximum(values, 0.0) + log_shifted


def joined(stats):
    peaks, totals, targets = (stats[:, k : k + 1] for k in range(3))
    row_peak = jnp.max(peaks, axis=0)
    row_total = jnp.sum(totals * jnp.exp(peaks - row_peak[None]), axis=0)
    window_lse = row_peak + jnp.log(row_total)
    outside = stats[0, 3:4]
    ceiling = jnp.maximum(window_lse, outside)
    full_lse = ceiling + jnp.log(jnp.exp(window_lse - ceiling) + jnp.exp(outside - ceiling))
    return full_lse, jnp.sum(targets, axis=0)


def preference(full_lse, target_logit, live, prior, share, pair_count):
    tokens = live.shape[1]
    sequence = lax.broadcasted_iota(jnp.int32, live.shape, 1) // (tokens // (2 * pair_count))
    token_logp = live * (target_logit - full_lse)
    token_grad = jnp.zeros(live.shape, jnp.float32)
    loss = jnp.zeros((1, 1), jnp.float32)

    def of_sequence(values, here):
        return jnp.sum(jnp.where(here, values, 0.0), axis=1, keepdims=True)

    def first_of(values, here):
        return jnp.max(jnp.where(here, values, -jnp.inf), axis=1, keepdims=True)

    for pair in range(pair_count):
        chosen, rejected = (sequence == 2 * pair + one for one in range(2))
        margin = beta_scale * (
            (of_sequence(token_logp, chosen) - first_of(prior, chosen))
            - (of_sequence(token_logp, rejected) - first_of(prior, rejected))
        )
        pair_share = first_of(share, chosen)
        loss += pair_share * softplus(-margin)
        coefficient = -beta_scale * pair_share / (1.0 + jnp.exp(margin))
        token_grad += jnp.where(chosen, coefficient, 0.0) - jnp.where(rejected, coefficient, 0.0)
    return loss, live * token_grad


def rows_kernel(
    pair_count, stats_ref, own_ref, scaled_ref, matches_ref, weight_ref, rows_ref, loss_ref, grads_ref, made_ref, sems
):
    holders = weight_ref.shape[0]
    own_core = lax.axis_index("dp") % cores
    mine = pl.ds(pl.multiple_of(own_core * holders, holders), holders)
    full_lse, _ = joined(stats_ref[mine])
    scale = jnp.exp(own_ref[0:1] - full_lse)
    both = stacked_parts((matches_ref[...] - scale * scaled_ref[...]).T)
    sent = []
    for k in range(holders):
        made_ref[k] = product(both, weight_ref[holder_of(k, own_core)], 1)
        sent.append(pltpu.make_async_copy(made_ref.at[k], rows_ref.at[k], sems.at[k]))
        sent[k].start()
    loss = jnp.zeros((1, 1), jnp.float32)
    token_grad = jnp.zeros(loss_ref.shape, jnp.float32)
    for core in range(cores):
        stats = stats_ref[pl.ds(core * holders, holders)]
        given = (stats[0, k : k + 1] for k in range(4, 7))
        core_loss, core_grad = preference(*joined(stats), *given, pair_count)
        loss += core_loss
        token_grad = jnp.where(own_core == core, core_grad, token_grad)
    loss_ref[...] = jnp.broadcast_to(loss, loss_ref.shape)
    grads_ref[...] = jnp.broadcast_to(token_grad, grads_ref.shape[::-1]).T
    for copy in sent:
        copy.wait()


def gradient_rows(pair_count, stats, own, scaled, matches, weight_blocks):
    holders, width, columns = weight_blocks.shape
    tokens = own.shape[1]
    rows_shape = (holders, tokens, width)
    in_vmem = pl.BlockSpec(memory_space=pltpu.VMEM)
    return pl.pallas_call(
        functools.partial(rows_kernel, pair_count),
        out_shape=(
            pltpu.HBM(rows_shape, jnp.float32),
            jax.ShapeDtypeStruct((1, tokens), jnp.float32),
            jax.ShapeDtypeStruct((tokens, width), jnp.float32),
        ),
        in_specs=[in_vmem] * 5,
        out_specs=(pl.BlockSpec(memory_space=pltpu.HBM), in_vmem, in_vmem),
        scratch_shapes=[pltpu.VMEM(rows_shape, jnp.float32), pltpu.SemaphoreType.DMA((holders,))],
        compiler_params=pltpu.CompilerParams(vmem_limit_bytes=vmem_grant),
        cost_estimate=pl.CostEstimate(
            flops=6 * tokens * weight_blocks.size,
            bytes_accessed=4 * (holders * tokens * width + weight_blocks.size),
            transcendentals=tokens * holders,
        ),
        name="gradient_rows",
    )(stats, own, scaled, matches, weight_blocks)


def line_sum_kernel(parts_ref, loss_ref, sums_ref, passed_ref, made_ref, sems):
    passed_ref[...] = loss_ref[...]
    sent = []
    for k in range(made_ref.shape[0]):
        made_ref[k] = jnp.sum(parts_ref[:, k], axis=0)
        sent.append(pltpu.make_async_copy(made_ref.at[k], sums_ref.at[k], sems.at[k]))
        sent[k].start()
    for copy in sent:
        copy.wait()


def line_sums(parts, loss_row):
    shape = parts.shape[1:]
    in_vmem = pl.BlockSpec(memory_space=pltpu.VMEM)
    return pl.pallas_call(
        line_sum_kernel,
        out_shape=(
            pltpu.HBM(shape, jnp.float32),
            jax.ShapeDtypeStruct(loss_row.shape, jnp.float32),
        ),
        in_specs=[in_vmem] * 2,
        out_specs=(pl.BlockSpec(memory_space=pltpu.HBM), in_vmem),
        scratch_shapes=[pltpu.VMEM(shape, jnp.float32), pltpu.SemaphoreType.DMA((shape[0],))],
        compiler_params=pltpu.CompilerParams(vmem_limit_bytes=vmem_grant),
        name="line_sums",
    )(parts, loss_row)


def exchanged(blocks, groups):
    return lax.all_to_all(blocks, both_axes, 0, 0, axis_index_groups=groups, tiled=True)


def shards(hidden, head_weight, targets, lengths, rest_lse, ref_logp, group_map, group_weight):
    pair_count, _, seq_slots, local_width = hidden.shape
    pairs, holders = lax.axis_size("dp"), lax.axis_size("vocab")
    tokens = pair_count * 2 * seq_slots
    weight_blocks = head_weight.reshape(holders, local_width, -1)

    first_lines = line_groups(pairs, holders, True)
    second_lines = line_groups(pairs, holders, False)

    near = exchanged(copies_for_all(hidden.reshape(tokens, local_width), side), first_lines)
    states = exchanged(jnp.broadcast_to(near, (side, *near.shape)), second_lines)
    states = states.reshape(holders, tokens, local_width)
    scaled, matches, own_stats, stat_copies = local_logits(
        (lengths, ref_logp, group_map, group_weight), targets, rest_lse, states, weight_blocks
    )
    stats = exchanged(stat_copies, chip_plane_groups(pairs, holders))
    partial_rows, loss_row, token_grads = gradient_rows(
        pair_count, stats, own_stats, scaled, matches, weight_blocks
    )
    line_parts = exchanged(
        partial_rows.reshape(side, side, tokens, local_width), second_lines
    )
    loss_row = lax.psum(loss_row, both_axes, axis_index_groups=far_groups(pairs, holders))
    line_rows, loss_row = line_sums(line_parts, loss_row)
    summed_rows = jnp.sum(exchanged(line_rows, first_lines), axis=0)
    loss_row = lax.psum(loss_row, both_axes, axis_index_groups=near_groups(pairs, holders))
    return ((token_grads * summed_rows).reshape(hidden.shape), loss_row[0, 0])


def solution(mesh):
    return jax.shard_map(
        shards,
        mesh=mesh,
        in_specs=(
            P("dp", None, None, "vocab"),
            P(None, "vocab"),
            P("dp", None, None),
            P("dp", None),
            P("dp", None, None),
            P("dp", None),
            P("dp"),
            P(),
        ),
        out_specs=(P("dp", None, None, "vocab"), P()),
        check_vma=False,
    )
```

```python
import functools

import jax
import jax.numpy as jnp
from jax import lax
from jax.experimental import pallas as pl
from jax.experimental.pallas import tpu as pltpu
from jax.sharding import PartitionSpec as P

beta_scale = 0.05
both_axes = ("dp", "vocab")
cores = 2
side = 4
near_chips = 4
stat_rows = 8
vmem_grant = 24 * 1024 * 1024


def line_groups(pairs, holders, first):
    groups = []
    for pair in range(pairs):
        along_x = (pair % cores == 0) == first
        for line in range(side):
            places = [line * side + k if along_x else k * side + line for k in range(side)]
            groups.append([pair * holders + place for place in places])
    return groups


def chip_plane_groups(pairs, holders):
    return [
        [pair * holders + place for pair in (first, first + 1) for place in range(holders)]
        for first in range(0, pairs, cores)
    ]


def near_groups(pairs, holders):
    block = cores * near_chips
    return [
        [(start + k) * holders + place for k in range(0, block, cores)]
        for first in range(0, pairs, block)
        for start in range(first, first + cores)
        for place in range(holders)
    ]


def far_groups(pairs, holders):
    block = cores * near_chips
    return [
        [(first + k) * holders + place for first in range(0, pairs, block)]
        for k in range(block)
        for place in range(holders)
    ]


def split_parts(values):
    high = values.astype(jnp.bfloat16)
    low = (values - high.astype(jnp.float32)).astype(jnp.bfloat16)
    return high, low


def stacked_parts(values):
    return jnp.concatenate(split_parts(values), axis=0)


def product(both, weight, weight_dim):
    rows = both.shape[0] // 2
    high, low = split_parts(weight)
    dims = (((1,), (weight_dim,)), ((), ()))
    wide = lax.dot_general(both, high, dims, preferred_element_type=jnp.float32)
    narrow = lax.dot_general(both[:rows], low, dims, preferred_element_type=jnp.float32)
    return wide[:rows] + (wide[rows:] + narrow)


def column_matches(target_row, base, columns):
    ids = base + lax.broadcasted_iota(jnp.int32, (columns, target_row.shape[1]), 0)
    return ids == target_row


def holder_of(block, own_core):
    return jnp.where(own_core == 0, block, (block % side) * side + block // side)


def copies_kernel(shard_ref, out_ref):
    shard = shard_ref[...]
    for k in range(out_ref.shape[0]):
        out_ref[k] = shard


def copies_for_all(shard, holders):
    return pl.pallas_call(
        copies_kernel,
        out_shape=jax.ShapeDtypeStruct((holders, *shard.shape), shard.dtype),
        in_specs=[pl.BlockSpec(memory_space=pltpu.VMEM)],
        out_specs=pl.BlockSpec(memory_space=pltpu.VMEM),
        compiler_params=pltpu.CompilerParams(vmem_limit_bytes=vmem_grant),
        name="state_copies",
    )(shard)


def token_row(values_ref):
    pairs, ones, _ = values_ref.shape
    pieces = [values_ref[pair, one : one + 1] for pair in range(pairs) for one in range(ones)]
    return jnp.concatenate(pieces, axis=1)


def logits_kernel(
    lengths_ref,
    ref_logp_ref,
    group_map_ref,
    weight_of_ref,
    targets_ref,
    rest_lse_ref,
    states_ref,
    weight_ref,
    scaled_ref,
    matches_ref,
    own_ref,
    stats_ref,
):
    pair_count, _, seq_slots = targets_ref.shape
    target_row = token_row(targets_ref)
    token = lax.broadcasted_iota(jnp.int32, target_row.shape, 1)
    slot, sequence = token % seq_slots, token // seq_slots
    divisor = 0.0
    for k in range(weight_of_ref.shape[0]):
        divisor += weight_of_ref[k]
    divisor = pair_count * divisor
    live = jnp.zeros(target_row.shape, jnp.float32)
    prior = jnp.zeros(target_row.shape, jnp.float32)
    share = jnp.zeros(target_row.shape, jnp.float32)
    for pair in range(pair_count):
        pair_share = weight_of_ref[group_map_ref[pair]]
        for one in range(2):
            here = sequence == 2 * pair + one
            live = jnp.where(here & (slot < lengths_ref[pair, one]), 1.0, live)
            prior = jnp.where(here, ref_logp_ref[pair, one], prior)
            share = jnp.where(here, pair_share, share)
    share = share / divisor

    own_core = lax.axis_index("dp") % cores
    total = product(stacked_parts(states_ref[0]), weight_ref[0], 0)
    for k in range(1, states_ref.shape[0]):
        total += product(stacked_parts(states_ref[k]), weight_ref[holder_of(k, own_core)], 0)
    logits = total.T
    peak = jnp.max(logits, axis=0, keepdims=True)
    scaled = jnp.exp(logits - peak)
    scaled_ref[...] = scaled
    ids = lax.axis_index("vocab") * logits.shape[0] + lax.broadcasted_iota(jnp.int32, logits.shape, 0)
    matches = ids == target_row
    matches_ref[...] = matches.astype(jnp.float32)
    exponentials = jnp.sum(scaled, axis=0, keepdims=True)
    target = jnp.sum(jnp.where(matches, logits, 0.0), axis=0, keepdims=True)
    row = lax.broadcasted_iota(jnp.int32, own_ref.shape, 0)
    stats = jnp.zeros(own_ref.shape, jnp.float32)
    for k, values in enumerate((peak, exponentials, target, token_row(rest_lse_ref), live, prior, share)):
        stats = jnp.where(row == k, values, stats)
    own_ref[...] = stats
    for k in range(stats_ref.shape[0]):
        stats_ref[k] = stats


def local_logits(scalars, targets, rest_lse, states, weight_blocks):
    holders, tokens, _ = states.shape
    columns = weight_blocks.shape[2]
    in_vmem = pl.BlockSpec(memory_space=pltpu.VMEM)
    return pl.pallas_call(
        logits_kernel,
        out_shape=(
            jax.ShapeDtypeStruct((columns, tokens), jnp.float32),
            jax.ShapeDtypeStruct((columns, tokens), jnp.float32),
            jax.ShapeDtypeStruct((stat_rows, tokens), jnp.float32),
            jax.ShapeDtypeStruct((cores * holders, stat_rows, tokens), jnp.float32),
        ),
        in_specs=[pl.BlockSpec(memory_space=pltpu.SMEM)] * len(scalars) + [in_vmem] * 4,
        out_specs=(in_vmem,) * 4,
        compiler_params=pltpu.CompilerParams(vmem_limit_bytes=vmem_grant),
        cost_estimate=pl.CostEstimate(
            flops=6 * states.size * columns,
            bytes_accessed=4 * (states.size + weight_blocks.size),
            transcendentals=tokens * columns,
        ),
        name="local_logits",
    )(*scalars, targets, rest_lse, states, weight_blocks)


def softplus(values):
    small = jnp.exp(-jnp.abs(values))
    shifted = 1.0 + small
    gap = shifted - 1.0
    safe = jnp.where(gap == 0.0, 1.0, gap)
    log_shifted = jnp.where(gap == 0.0, small, jnp.log(shifted) * (small / safe))
    return jnp.maximum(values, 0.0) + log_shifted


def joined(stats):
    peaks, totals, targets = (stats[:, k : k + 1] for k in range(3))
    row_peak = jnp.max(peaks, axis=0)
    row_total = jnp.sum(totals * jnp.exp(peaks - row_peak[None]), axis=0)
    window_lse = row_peak + jnp.log(row_total)
    outside = stats[0, 3:4]
    ceiling = jnp.maximum(window_lse, outside)
    full_lse = ceiling + jnp.log(jnp.exp(window_lse - ceiling) + jnp.exp(outside - ceiling))
    return full_lse, jnp.sum(targets, axis=0)


def preference(full_lse, target_logit, live, prior, share, pair_count):
    tokens = live.shape[1]
    sequence = lax.broadcasted_iota(jnp.int32, live.shape, 1) // (tokens // (2 * pair_count))
    token_logp = live * (target_logit - full_lse)
    token_grad = jnp.zeros(live.shape, jnp.float32)
    loss = jnp.zeros((1, 1), jnp.float32)

    def of_sequence(values, here):
        return jnp.sum(jnp.where(here, values, 0.0), axis=1, keepdims=True)

    def first_of(values, here):
        return jnp.max(jnp.where(here, values, -jnp.inf), axis=1, keepdims=True)

    for pair in range(pair_count):
        chosen, rejected = (sequence == 2 * pair + one for one in range(2))
        margin = beta_scale * (
            (of_sequence(token_logp, chosen) - first_of(prior, chosen))
            - (of_sequence(token_logp, rejected) - first_of(prior, rejected))
        )
        pair_share = first_of(share, chosen)
        loss += pair_share * softplus(-margin)
        coefficient = -beta_scale * pair_share / (1.0 + jnp.exp(margin))
        token_grad += jnp.where(chosen, coefficient, 0.0) - jnp.where(rejected, coefficient, 0.0)
    return loss, live * token_grad


def rows_kernel(
    pair_count, stats_ref, own_ref, scaled_ref, matches_ref, weight_ref, rows_ref, loss_ref, grads_ref, made_ref, sems
):
    holders = weight_ref.shape[0]
    own_core = lax.axis_index("dp") % cores
    mine = pl.ds(pl.multiple_of(own_core * holders, holders), holders)
    full_lse, _ = joined(stats_ref[mine])
    scale = jnp.exp(own_ref[0:1] - full_lse)
    both = stacked_parts((matches_ref[...] - scale * scaled_ref[...]).T)
    sent = []
    for k in range(holders):
        made_ref[k] = product(both, weight_ref[holder_of(k, own_core)], 1)
        sent.append(pltpu.make_async_copy(made_ref.at[k], rows_ref.at[k], sems.at[k]))
        sent[k].start()
    loss = jnp.zeros((1, 1), jnp.float32)
    token_grad = jnp.zeros(loss_ref.shape, jnp.float32)
    for core in range(cores):
        stats = stats_ref[pl.ds(core * holders, holders)]
        given = (stats[0, k : k + 1] for k in range(4, 7))
        core_loss, core_grad = preference(*joined(stats), *given, pair_count)
        loss += core_loss
        token_grad = jnp.where(own_core == core, core_grad, token_grad)
    loss_ref[...] = jnp.broadcast_to(loss, loss_ref.shape)
    grads_ref[...] = jnp.broadcast_to(token_grad, grads_ref.shape[::-1]).T
    for copy in sent:
        copy.wait()


def gradient_rows(pair_count, stats, own, scaled, matches, weight_blocks):
    holders, width, columns = weight_blocks.shape
    tokens = own.shape[1]
    rows_shape = (holders, tokens, width)
    in_vmem = pl.BlockSpec(memory_space=pltpu.VMEM)
    return pl.pallas_call(
        functools.partial(rows_kernel, pair_count),
        out_shape=(
            pltpu.HBM(rows_shape, jnp.float32),
            jax.ShapeDtypeStruct((1, tokens), jnp.float32),
            jax.ShapeDtypeStruct((tokens, width), jnp.float32),
        ),
        in_specs=[in_vmem] * 5,
        out_specs=(pl.BlockSpec(memory_space=pltpu.HBM), in_vmem, in_vmem),
        scratch_shapes=[pltpu.VMEM(rows_shape, jnp.float32), pltpu.SemaphoreType.DMA((holders,))],
        compiler_params=pltpu.CompilerParams(vmem_limit_bytes=vmem_grant),
        cost_estimate=pl.CostEstimate(
            flops=6 * tokens * weight_blocks.size,
            bytes_accessed=4 * (holders * tokens * width + weight_blocks.size),
            transcendentals=tokens * holders,
        ),
        name="gradient_rows",
    )(stats, own, scaled, matches, weight_blocks)


def line_sum_kernel(parts_ref, losses_ref, sums_ref, loss_ref, made_ref, sems):
    loss_ref[...] = jnp.sum(losses_ref[...], axis=0, keepdims=True)
    sent = []
    for k in range(made_ref.shape[0]):
        made_ref[k] = jnp.sum(parts_ref[:, k], axis=0)
        sent.append(pltpu.make_async_copy(made_ref.at[k], sums_ref.at[k], sems.at[k]))
        sent[k].start()
    for copy in sent:
        copy.wait()


def line_sums(parts, loss_rows):
    shape = parts.shape[1:]
    in_vmem = pl.BlockSpec(memory_space=pltpu.VMEM)
    return pl.pallas_call(
        line_sum_kernel,
        out_shape=(
            pltpu.HBM(shape, jnp.float32),
            jax.ShapeDtypeStruct((1, loss_rows.shape[1]), jnp.float32),
        ),
        in_specs=[in_vmem] * 2,
        out_specs=(pl.BlockSpec(memory_space=pltpu.HBM), in_vmem),
        scratch_shapes=[pltpu.VMEM(shape, jnp.float32), pltpu.SemaphoreType.DMA((shape[0],))],
        compiler_params=pltpu.CompilerParams(vmem_limit_bytes=vmem_grant),
        name="line_sums",
    )(parts, loss_rows)


def exchanged(blocks, groups):
    return lax.all_to_all(blocks, both_axes, 0, 0, axis_index_groups=groups, tiled=True)


def gathered(row, groups):
    return lax.all_gather(row, both_axes, axis_index_groups=groups, axis=0, tiled=True)


def shards(hidden, head_weight, targets, lengths, rest_lse, ref_logp, group_map, group_weight):
    pair_count, _, seq_slots, local_width = hidden.shape
    pairs, holders = lax.axis_size("dp"), lax.axis_size("vocab")
    tokens = pair_count * 2 * seq_slots
    weight_blocks = head_weight.reshape(holders, local_width, -1)

    first_lines = line_groups(pairs, holders, True)
    second_lines = line_groups(pairs, holders, False)

    near = exchanged(copies_for_all(hidden.reshape(tokens, local_width), side), first_lines)
    states = exchanged(jnp.broadcast_to(near, (side, *near.shape)), second_lines)
    states = states.reshape(holders, tokens, local_width)
    scaled, matches, own_stats, stat_copies = local_logits(
        (lengths, ref_logp, group_map, group_weight), targets, rest_lse, states, weight_blocks
    )
    stats = exchanged(stat_copies, chip_plane_groups(pairs, holders))
    partial_rows, loss_row, token_grads = gradient_rows(
        pair_count, stats, own_stats, scaled, matches, weight_blocks
    )
    line_parts = exchanged(
        partial_rows.reshape(side, side, tokens, local_width), second_lines
    )
    far_rows = gathered(loss_row, far_groups(pairs, holders))
    line_rows, loss_row = line_sums(line_parts, far_rows)
    summed_rows = jnp.sum(exchanged(line_rows, first_lines), axis=0)
    near_rows = gathered(loss_row, near_groups(pairs, holders))
    dpo_loss = jnp.sum(near_rows, axis=0)[0]
    return ((token_grads * summed_rows).reshape(hidden.shape), dpo_loss)


def solution(mesh):
    return jax.shard_map(
        shards,
        mesh=mesh,
        in_specs=(
            P("dp", None, None, "vocab"),
            P(None, "vocab"),
            P("dp", None, None),
            P("dp", None),
            P("dp", None, None),
            P("dp", None),
            P("dp"),
            P(),
        ),
        out_specs=(P("dp", None, None, "vocab"), P()),
        check_vma=False,
    )
```

```python
import functools

import jax
import jax.numpy as jnp
from jax import lax
from jax.experimental import pallas as pl
from jax.experimental.pallas import tpu as pltpu
from jax.sharding import PartitionSpec as P

beta_scale = 0.05
both_axes = ("dp", "vocab")
cores = 2
side = 4
near_chips = 4
stat_rows = 8
vmem_grant = 24 * 1024 * 1024


def line_groups(pairs, holders, first):
    groups = []
    for pair in range(pairs):
        along_x = (pair % cores == 0) == first
        for line in range(side):
            places = [line * side + k if along_x else k * side + line for k in range(side)]
            groups.append([pair * holders + place for place in places])
    return groups


def plane_groups(pairs, holders):
    swapped = [(place % side) * side + place // side for place in range(holders)]
    return [
        [pair * holders + place for place in (range(holders) if pair % cores == 0 else swapped)]
        for pair in range(pairs)
    ]


def chip_plane_groups(pairs, holders):
    return [
        [pair * holders + place for pair in (first, first + 1) for place in range(holders)]
        for first in range(0, pairs, cores)
    ]


def near_groups(pairs, holders):
    block = cores * near_chips
    return [
        [(start + k) * holders + place for k in range(0, block, cores)]
        for first in range(0, pairs, block)
        for start in range(first, first + cores)
        for place in range(holders)
    ]


def far_groups(pairs, holders):
    block = cores * near_chips
    return [
        [(first + k) * holders + place for first in range(0, pairs, block)]
        for k in range(block)
        for place in range(holders)
    ]


def split_parts(values):
    high = values.astype(jnp.bfloat16)
    low = (values - high.astype(jnp.float32)).astype(jnp.bfloat16)
    return high, low


def stacked_parts(values):
    return jnp.concatenate(split_parts(values), axis=0)


def product(both, weight, weight_dim):
    rows = both.shape[0] // 2
    high, low = split_parts(weight)
    dims = (((1,), (weight_dim,)), ((), ()))
    wide = lax.dot_general(both, high, dims, preferred_element_type=jnp.float32)
    narrow = lax.dot_general(both[:rows], low, dims, preferred_element_type=jnp.float32)
    return wide[:rows] + (wide[rows:] + narrow)


def column_matches(target_row, base, columns):
    ids = base + lax.broadcasted_iota(jnp.int32, (columns, target_row.shape[1]), 0)
    return ids == target_row


def holder_of(block, own_core):
    return jnp.where(own_core == 0, block, (block % side) * side + block // side)


def copies_kernel(shard_ref, out_ref):
    shard = shard_ref[...]
    for k in range(out_ref.shape[0]):
        out_ref[k] = shard


def copies_for_all(shard, holders):
    return pl.pallas_call(
        copies_kernel,
        out_shape=jax.ShapeDtypeStruct((holders, *shard.shape), shard.dtype),
        in_specs=[pl.BlockSpec(memory_space=pltpu.VMEM)],
        out_specs=pl.BlockSpec(memory_space=pltpu.VMEM),
        compiler_params=pltpu.CompilerParams(vmem_limit_bytes=vmem_grant),
        name="state_copies",
    )(shard)


def token_row(values_ref):
    pairs, ones, _ = values_ref.shape
    pieces = [values_ref[pair, one : one + 1] for pair in range(pairs) for one in range(ones)]
    return jnp.concatenate(pieces, axis=1)


def logits_kernel(
    lengths_ref,
    ref_logp_ref,
    group_map_ref,
    weight_of_ref,
    targets_ref,
    rest_lse_ref,
    states_ref,
    weight_ref,
    scaled_ref,
    matches_ref,
    own_ref,
    stats_ref,
):
    pair_count, _, seq_slots = targets_ref.shape
    target_row = token_row(targets_ref)
    token = lax.broadcasted_iota(jnp.int32, target_row.shape, 1)
    slot, sequence = token % seq_slots, token // seq_slots
    divisor = 0.0
    for k in range(weight_of_ref.shape[0]):
        divisor += weight_of_ref[k]
    divisor = pair_count * divisor
    live = jnp.zeros(target_row.shape, jnp.float32)
    prior = jnp.zeros(target_row.shape, jnp.float32)
    share = jnp.zeros(target_row.shape, jnp.float32)
    for pair in range(pair_count):
        pair_share = weight_of_ref[group_map_ref[pair]]
        for one in range(2):
            here = sequence == 2 * pair + one
            live = jnp.where(here & (slot < lengths_ref[pair, one]), 1.0, live)
            prior = jnp.where(here, ref_logp_ref[pair, one], prior)
            share = jnp.where(here, pair_share, share)
    share = share / divisor

    own_core = lax.axis_index("dp") % cores
    total = product(stacked_parts(states_ref[0]), weight_ref[0], 0)
    for k in range(1, states_ref.shape[0]):
        total += product(stacked_parts(states_ref[k]), weight_ref[holder_of(k, own_core)], 0)
    logits = total.T
    peak = jnp.max(logits, axis=0, keepdims=True)
    scaled = jnp.exp(logits - peak)
    scaled_ref[...] = scaled
    ids = lax.axis_index("vocab") * logits.shape[0] + lax.broadcasted_iota(jnp.int32, logits.shape, 0)
    matches = ids == target_row
    matches_ref[...] = matches.astype(jnp.float32)
    exponentials = jnp.sum(scaled, axis=0, keepdims=True)
    target = jnp.sum(jnp.where(matches, logits, 0.0), axis=0, keepdims=True)
    row = lax.broadcasted_iota(jnp.int32, own_ref.shape, 0)
    stats = jnp.zeros(own_ref.shape, jnp.float32)
    for k, values in enumerate((peak, exponentials, target, token_row(rest_lse_ref), live, prior, share)):
        stats = jnp.where(row == k, values, stats)
    own_ref[...] = stats
    for k in range(stats_ref.shape[0]):
        stats_ref[k] = stats


def local_logits(scalars, targets, rest_lse, states, weight_blocks):
    holders, tokens, _ = states.shape
    columns = weight_blocks.shape[2]
    in_vmem = pl.BlockSpec(memory_space=pltpu.VMEM)
    return pl.pallas_call(
        logits_kernel,
        out_shape=(
            jax.ShapeDtypeStruct((columns, tokens), jnp.float32),
            jax.ShapeDtypeStruct((columns, tokens), jnp.float32),
            jax.ShapeDtypeStruct((stat_rows, tokens), jnp.float32),
            jax.ShapeDtypeStruct((cores * holders, stat_rows, tokens), jnp.float32),
        ),
        in_specs=[pl.BlockSpec(memory_space=pltpu.SMEM)] * len(scalars) + [in_vmem] * 4,
        out_specs=(in_vmem,) * 4,
        compiler_params=pltpu.CompilerParams(vmem_limit_bytes=vmem_grant),
        cost_estimate=pl.CostEstimate(
            flops=6 * states.size * columns,
            bytes_accessed=4 * (states.size + weight_blocks.size),
            transcendentals=tokens * columns,
        ),
        name="local_logits",
    )(*scalars, targets, rest_lse, states, weight_blocks)


def softplus(values):
    small = jnp.exp(-jnp.abs(values))
    shifted = 1.0 + small
    gap = shifted - 1.0
    safe = jnp.where(gap == 0.0, 1.0, gap)
    log_shifted = jnp.where(gap == 0.0, small, jnp.log(shifted) * (small / safe))
    return jnp.maximum(values, 0.0) + log_shifted


def joined(stats):
    peaks, totals, targets = (stats[:, k : k + 1] for k in range(3))
    row_peak = jnp.max(peaks, axis=0)
    row_total = jnp.sum(totals * jnp.exp(peaks - row_peak[None]), axis=0)
    window_lse = row_peak + jnp.log(row_total)
    outside = stats[0, 3:4]
    ceiling = jnp.maximum(window_lse, outside)
    full_lse = ceiling + jnp.log(jnp.exp(window_lse - ceiling) + jnp.exp(outside - ceiling))
    return full_lse, jnp.sum(targets, axis=0)


def preference(full_lse, target_logit, live, prior, share, pair_count):
    tokens = live.shape[1]
    sequence = lax.broadcasted_iota(jnp.int32, live.shape, 1) // (tokens // (2 * pair_count))
    token_logp = live * (target_logit - full_lse)
    token_grad = jnp.zeros(live.shape, jnp.float32)
    loss = jnp.zeros((1, 1), jnp.float32)

    def of_sequence(values, here):
        return jnp.sum(jnp.where(here, values, 0.0), axis=1, keepdims=True)

    def first_of(values, here):
        return jnp.max(jnp.where(here, values, -jnp.inf), axis=1, keepdims=True)

    for pair in range(pair_count):
        chosen, rejected = (sequence == 2 * pair + one for one in range(2))
        margin = beta_scale * (
            (of_sequence(token_logp, chosen) - first_of(prior, chosen))
            - (of_sequence(token_logp, rejected) - first_of(prior, rejected))
        )
        pair_share = first_of(share, chosen)
        loss += pair_share * softplus(-margin)
        coefficient = -beta_scale * pair_share / (1.0 + jnp.exp(margin))
        token_grad += jnp.where(chosen, coefficient, 0.0) - jnp.where(rejected, coefficient, 0.0)
    return loss, live * token_grad


def rows_kernel(
    pair_count, stats_ref, own_ref, scaled_ref, matches_ref, weight_ref, rows_ref, loss_ref, grads_ref, made_ref, sems
):
    holders = weight_ref.shape[0]
    own_core = lax.axis_index("dp") % cores
    mine = pl.ds(pl.multiple_of(own_core * holders, holders), holders)
    full_lse, _ = joined(stats_ref[mine])
    scale = jnp.exp(own_ref[0:1] - full_lse)
    both = stacked_parts((matches_ref[...] - scale * scaled_ref[...]).T)
    sent = []
    for k in range(holders):
        made_ref[k] = product(both, weight_ref[holder_of(k, own_core)], 1)
        sent.append(pltpu.make_async_copy(made_ref.at[k], rows_ref.at[k], sems.at[k]))
        sent[k].start()
    loss = jnp.zeros((1, 1), jnp.float32)
    token_grad = jnp.zeros(loss_ref.shape, jnp.float32)
    for core in range(cores):
        stats = stats_ref[pl.ds(core * holders, holders)]
        given = (stats[0, k : k + 1] for k in range(4, 7))
        core_loss, core_grad = preference(*joined(stats), *given, pair_count)
        loss += core_loss
        token_grad = jnp.where(own_core == core, core_grad, token_grad)
    loss_ref[...] = jnp.broadcast_to(loss, loss_ref.shape)
    grads_ref[...] = jnp.broadcast_to(token_grad, grads_ref.shape[::-1]).T
    for copy in sent:
        copy.wait()


def gradient_rows(pair_count, stats, own, scaled, matches, weight_blocks):
    holders, width, columns = weight_blocks.shape
    tokens = own.shape[1]
    rows_shape = (holders, tokens, width)
    in_vmem = pl.BlockSpec(memory_space=pltpu.VMEM)
    return pl.pallas_call(
        functools.partial(rows_kernel, pair_count),
        out_shape=(
            pltpu.HBM(rows_shape, jnp.float32),
            jax.ShapeDtypeStruct((1, tokens), jnp.float32),
            jax.ShapeDtypeStruct((tokens, width), jnp.float32),
        ),
        in_specs=[in_vmem] * 5,
        out_specs=(pl.BlockSpec(memory_space=pltpu.HBM), in_vmem, in_vmem),
        scratch_shapes=[pltpu.VMEM(rows_shape, jnp.float32), pltpu.SemaphoreType.DMA((holders,))],
        compiler_params=pltpu.CompilerParams(vmem_limit_bytes=vmem_grant),
        cost_estimate=pl.CostEstimate(
            flops=6 * tokens * weight_blocks.size,
            bytes_accessed=4 * (holders * tokens * width + weight_blocks.size),
            transcendentals=tokens * holders,
        ),
        name="gradient_rows",
    )(stats, own, scaled, matches, weight_blocks)


def exchanged(blocks, groups):
    return lax.all_to_all(blocks, both_axes, 0, 0, axis_index_groups=groups, tiled=True)


def gathered(row, groups):
    return lax.all_gather(row, both_axes, axis_index_groups=groups, axis=0, tiled=True)


def shards(hidden, head_weight, targets, lengths, rest_lse, ref_logp, group_map, group_weight):
    pair_count, _, seq_slots, local_width = hidden.shape
    pairs, holders = lax.axis_size("dp"), lax.axis_size("vocab")
    tokens = pair_count * 2 * seq_slots
    weight_blocks = head_weight.reshape(holders, local_width, -1)

    first_lines = line_groups(pairs, holders, True)
    second_lines = line_groups(pairs, holders, False)

    near = exchanged(copies_for_all(hidden.reshape(tokens, local_width), side), first_lines)
    states = exchanged(jnp.broadcast_to(near, (side, *near.shape)), second_lines)
    states = states.reshape(holders, tokens, local_width)
    scaled, matches, own_stats, stat_copies = local_logits(
        (lengths, ref_logp, group_map, group_weight), targets, rest_lse, states, weight_blocks
    )
    stats = exchanged(stat_copies, chip_plane_groups(pairs, holders))
    partial_rows, loss_row, token_grads = gradient_rows(
        pair_count, stats, own_stats, scaled, matches, weight_blocks
    )
    summed_rows = jnp.sum(exchanged(partial_rows, plane_groups(pairs, holders)), axis=0)
    far_rows = gathered(loss_row, far_groups(pairs, holders))
    loss_row = jnp.sum(far_rows, axis=0, keepdims=True)
    near_rows = gathered(loss_row, near_groups(pairs, holders))
    dpo_loss = jnp.sum(near_rows, axis=0)[0]
    return ((token_grads * summed_rows).reshape(hidden.shape), dpo_loss)


def solution(mesh):
    return jax.shard_map(
        shards,
        mesh=mesh,
        in_specs=(
            P("dp", None, None, "vocab"),
            P(None, "vocab"),
            P("dp", None, None),
            P("dp", None),
            P("dp", None, None),
            P("dp", None),
            P("dp"),
            P(),
        ),
        out_specs=(P("dp", None, None, "vocab"), P()),
        check_vma=False,
    )
```

```python
import functools

import jax
import jax.numpy as jnp
from jax import lax
from jax.experimental import pallas as pl
from jax.experimental.pallas import tpu as pltpu
from jax.sharding import PartitionSpec as P

beta_scale = 0.05
both_axes = ("dp", "vocab")
cores = 2
side = 4
near_chips = 4
stat_rows = 8
vmem_grant = 24 * 1024 * 1024


def line_groups(pairs, holders, first):
    groups = []
    for pair in range(pairs):
        along_x = (pair % cores == 0) == first
        for line in range(side):
            places = [line * side + k if along_x else k * side + line for k in range(side)]
            groups.append([pair * holders + place for place in places])
    return groups


def plane_groups(pairs, holders):
    swapped = [(place % side) * side + place // side for place in range(holders)]
    return [
        [pair * holders + place for place in (range(holders) if pair % cores == 0 else swapped)]
        for pair in range(pairs)
    ]


def chip_plane_groups(pairs, holders):
    return [
        [pair * holders + place for pair in (first, first + 1) for place in range(holders)]
        for first in range(0, pairs, cores)
    ]


def near_groups(pairs, holders):
    block = cores * near_chips
    return [
        [(start + k) * holders + place for k in range(0, block, cores)]
        for first in range(0, pairs, block)
        for start in range(first, first + cores)
        for place in range(holders)
    ]


def far_groups(pairs, holders):
    block = cores * near_chips
    return [
        [(first + k) * holders + place for first in range(0, pairs, block)]
        for k in range(block)
        for place in range(holders)
    ]


def split_parts(values):
    high = values.astype(jnp.bfloat16)
    low = (values - high.astype(jnp.float32)).astype(jnp.bfloat16)
    return high, low


def stacked_parts(values):
    return jnp.concatenate(split_parts(values), axis=0)


def product(both, weight, weight_dim):
    rows = both.shape[0] // 2
    high, low = split_parts(weight)
    dims = (((1,), (weight_dim,)), ((), ()))
    wide = lax.dot_general(both, high, dims, preferred_element_type=jnp.float32)
    narrow = lax.dot_general(both[:rows], low, dims, preferred_element_type=jnp.float32)
    return wide[:rows] + (wide[rows:] + narrow)


def column_matches(target_row, base, columns):
    ids = base + lax.broadcasted_iota(jnp.int32, (columns, target_row.shape[1]), 0)
    return ids == target_row


def holder_of(block, own_core):
    return jnp.where(own_core == 0, block, (block % side) * side + block // side)


def copies_kernel(shard_ref, out_ref):
    shard = shard_ref[...]
    for k in range(out_ref.shape[0]):
        out_ref[k] = shard


def copies_for_all(shard, holders):
    return pl.pallas_call(
        copies_kernel,
        out_shape=jax.ShapeDtypeStruct((holders, *shard.shape), shard.dtype),
        in_specs=[pl.BlockSpec(memory_space=pltpu.VMEM)],
        out_specs=pl.BlockSpec(memory_space=pltpu.VMEM),
        compiler_params=pltpu.CompilerParams(vmem_limit_bytes=vmem_grant),
        name="state_copies",
    )(shard)


def token_row(values_ref):
    pairs, ones, _ = values_ref.shape
    pieces = [values_ref[pair, one : one + 1] for pair in range(pairs) for one in range(ones)]
    return jnp.concatenate(pieces, axis=1)


def logits_kernel(
    lengths_ref,
    ref_logp_ref,
    group_map_ref,
    weight_of_ref,
    targets_ref,
    rest_lse_ref,
    states_ref,
    weight_ref,
    scaled_ref,
    matches_ref,
    own_ref,
    stats_ref,
):
    pair_count, _, seq_slots = targets_ref.shape
    target_row = token_row(targets_ref)
    token = lax.broadcasted_iota(jnp.int32, target_row.shape, 1)
    slot, sequence = token % seq_slots, token // seq_slots
    group_weights = weight_of_ref[...]
    group_ids = lax.broadcasted_iota(jnp.int32, group_weights.shape, 1)
    divisor = pair_count * jnp.sum(group_weights, axis=1, keepdims=True)
    count = jnp.zeros(target_row.shape, jnp.int32)
    prior = jnp.zeros(target_row.shape, jnp.float32)
    share = jnp.zeros(target_row.shape, jnp.float32)
    for pair in range(pair_count):
        chosen_group = group_ids == group_map_ref[0:1, pair : pair + 1]
        pair_weight = jnp.sum(jnp.where(chosen_group, group_weights, 0.0), axis=1, keepdims=True)
        share = jnp.where(sequence // 2 == pair, pair_weight / divisor, share)
        for one in range(2):
            here = sequence == 2 * pair + one
            count = jnp.where(here, lengths_ref[pair : pair + 1, one : one + 1], count)
            prior = jnp.where(here, ref_logp_ref[pair : pair + 1, one : one + 1], prior)
    live = jnp.where(slot < count, 1.0, 0.0)

    own_core = lax.axis_index("dp") % cores
    total = product(stacked_parts(states_ref[0]), weight_ref[0], 0)
    for k in range(1, states_ref.shape[0]):
        total += product(stacked_parts(states_ref[k]), weight_ref[holder_of(k, own_core)], 0)
    logits = total.T
    peak = jnp.max(logits, axis=0, keepdims=True)
    scaled = jnp.exp(logits - peak)
    scaled_ref[...] = scaled
    ids = lax.axis_index("vocab") * logits.shape[0] + lax.broadcasted_iota(jnp.int32, logits.shape, 0)
    matches = ids == target_row
    matches_ref[...] = matches.astype(jnp.float32)
    exponentials = jnp.sum(scaled, axis=0, keepdims=True)
    target = jnp.sum(jnp.where(matches, logits, 0.0), axis=0, keepdims=True)
    row = lax.broadcasted_iota(jnp.int32, own_ref.shape, 0)
    stats = jnp.zeros(own_ref.shape, jnp.float32)
    for k, values in enumerate((peak, exponentials, target, token_row(rest_lse_ref), live, prior, share)):
        stats = jnp.where(row == k, values, stats)
    own_ref[...] = stats
    for k in range(stats_ref.shape[0]):
        stats_ref[k] = stats


def local_logits(small, targets, rest_lse, states, weight_blocks):
    holders, tokens, _ = states.shape
    columns = weight_blocks.shape[2]
    in_vmem = pl.BlockSpec(memory_space=pltpu.VMEM)
    return pl.pallas_call(
        logits_kernel,
        out_shape=(
            jax.ShapeDtypeStruct((columns, tokens), jnp.float32),
            jax.ShapeDtypeStruct((columns, tokens), jnp.float32),
            jax.ShapeDtypeStruct((stat_rows, tokens), jnp.float32),
            jax.ShapeDtypeStruct((cores * holders, stat_rows, tokens), jnp.float32),
        ),
        in_specs=[in_vmem] * (len(small) + 4),
        out_specs=(in_vmem,) * 4,
        compiler_params=pltpu.CompilerParams(vmem_limit_bytes=vmem_grant),
        cost_estimate=pl.CostEstimate(
            flops=6 * states.size * columns,
            bytes_accessed=4 * (states.size + weight_blocks.size),
            transcendentals=tokens * columns,
        ),
        name="local_logits",
    )(*small, targets, rest_lse, states, weight_blocks)


def softplus(values):
    small = jnp.exp(-jnp.abs(values))
    shifted = 1.0 + small
    gap = shifted - 1.0
    safe = jnp.where(gap == 0.0, 1.0, gap)
    log_shifted = jnp.where(gap == 0.0, small, jnp.log(shifted) * (small / safe))
    return jnp.maximum(values, 0.0) + log_shifted


def joined(stats):
    peaks, totals, targets = (stats[:, k : k + 1] for k in range(3))
    row_peak = jnp.max(peaks, axis=0)
    row_total = jnp.sum(totals * jnp.exp(peaks - row_peak[None]), axis=0)
    window_lse = row_peak + jnp.log(row_total)
    outside = stats[0, 3:4]
    ceiling = jnp.maximum(window_lse, outside)
    full_lse = ceiling + jnp.log(jnp.exp(window_lse - ceiling) + jnp.exp(outside - ceiling))
    return full_lse, jnp.sum(targets, axis=0)


def preference(full_lse, target_logit, live, prior, share, pair_count):
    tokens = live.shape[1]
    sequence = lax.broadcasted_iota(jnp.int32, live.shape, 1) // (tokens // (2 * pair_count))
    token_logp = live * (target_logit - full_lse)
    token_grad = jnp.zeros(live.shape, jnp.float32)
    loss = jnp.zeros((1, 1), jnp.float32)

    def of_sequence(values, here):
        return jnp.sum(jnp.where(here, values, 0.0), axis=1, keepdims=True)

    def first_of(values, here):
        return jnp.max(jnp.where(here, values, -jnp.inf), axis=1, keepdims=True)

    for pair in range(pair_count):
        chosen, rejected = (sequence == 2 * pair + one for one in range(2))
        margin = beta_scale * (
            (of_sequence(token_logp, chosen) - first_of(prior, chosen))
            - (of_sequence(token_logp, rejected) - first_of(prior, rejected))
        )
        pair_share = first_of(share, chosen)
        loss += pair_share * softplus(-margin)
        coefficient = -beta_scale * pair_share / (1.0 + jnp.exp(margin))
        token_grad += jnp.where(chosen, coefficient, 0.0) - jnp.where(rejected, coefficient, 0.0)
    return loss, live * token_grad


def rows_kernel(
    pair_count, stats_ref, own_ref, scaled_ref, matches_ref, weight_ref, rows_ref, loss_ref, grads_ref, made_ref, sems
):
    holders = weight_ref.shape[0]
    own_core = lax.axis_index("dp") % cores
    mine = pl.ds(pl.multiple_of(own_core * holders, holders), holders)
    full_lse, _ = joined(stats_ref[mine])
    scale = jnp.exp(own_ref[0:1] - full_lse)
    both = stacked_parts((matches_ref[...] - scale * scaled_ref[...]).T)
    loss = jnp.zeros((1, 1), jnp.float32)
    token_grad = jnp.zeros(loss_ref.shape, jnp.float32)
    for core in range(cores):
        stats = stats_ref[pl.ds(core * holders, holders)]
        given = (stats[0, k : k + 1] for k in range(4, 7))
        core_loss, core_grad = preference(*joined(stats), *given, pair_count)
        loss += core_loss
        token_grad = jnp.where(own_core == core, core_grad, token_grad)
    loss_ref[...] = jnp.broadcast_to(loss, loss_ref.shape)
    grads_ref[...] = jnp.broadcast_to(token_grad, grads_ref.shape[::-1]).T
    sent = []
    for k in range(holders):
        made_ref[k] = product(both, weight_ref[holder_of(k, own_core)], 1)
        sent.append(pltpu.make_async_copy(made_ref.at[k], rows_ref.at[k], sems.at[k]))
        sent[k].start()
    for copy in sent:
        copy.wait()


def gradient_rows(pair_count, stats, own, scaled, matches, weight_blocks):
    holders, width, columns = weight_blocks.shape
    tokens = own.shape[1]
    rows_shape = (holders, tokens, width)
    in_vmem = pl.BlockSpec(memory_space=pltpu.VMEM)
    return pl.pallas_call(
        functools.partial(rows_kernel, pair_count),
        out_shape=(
            pltpu.HBM(rows_shape, jnp.float32),
            jax.ShapeDtypeStruct((1, tokens), jnp.float32),
            jax.ShapeDtypeStruct((tokens, width), jnp.float32),
        ),
        in_specs=[in_vmem] * 5,
        out_specs=(pl.BlockSpec(memory_space=pltpu.HBM), in_vmem, in_vmem),
        scratch_shapes=[pltpu.VMEM(rows_shape, jnp.float32), pltpu.SemaphoreType.DMA((holders,))],
        compiler_params=pltpu.CompilerParams(vmem_limit_bytes=vmem_grant),
        cost_estimate=pl.CostEstimate(
            flops=6 * tokens * weight_blocks.size,
            bytes_accessed=4 * (holders * tokens * width + weight_blocks.size),
            transcendentals=tokens * holders,
        ),
        name="gradient_rows",
    )(stats, own, scaled, matches, weight_blocks)


def exchanged(blocks, groups):
    return lax.all_to_all(blocks, both_axes, 0, 0, axis_index_groups=groups, tiled=True)


def gathered(row, groups):
    return lax.all_gather(row, both_axes, axis_index_groups=groups, axis=0, tiled=True)


def shards(hidden, head_weight, targets, lengths, rest_lse, ref_logp, group_map, group_weight):
    pair_count, _, seq_slots, local_width = hidden.shape
    pairs, holders = lax.axis_size("dp"), lax.axis_size("vocab")
    tokens = pair_count * 2 * seq_slots
    weight_blocks = head_weight.reshape(holders, local_width, -1)

    first_lines = line_groups(pairs, holders, True)
    second_lines = line_groups(pairs, holders, False)

    near = exchanged(copies_for_all(hidden.reshape(tokens, local_width), side), first_lines)
    states = exchanged(jnp.broadcast_to(near, (side, *near.shape)), second_lines)
    states = states.reshape(holders, tokens, local_width)
    scaled, matches, own_stats, stat_copies = local_logits(
        (lengths, ref_logp, group_map.reshape(1, -1), group_weight.reshape(1, -1)), targets, rest_lse, states, weight_blocks
    )
    stats = exchanged(stat_copies, chip_plane_groups(pairs, holders))
    partial_rows, loss_row, token_grads = gradient_rows(
        pair_count, stats, own_stats, scaled, matches, weight_blocks
    )
    summed_rows = jnp.sum(exchanged(partial_rows, plane_groups(pairs, holders)), axis=0)
    far_rows = gathered(loss_row, far_groups(pairs, holders))
    loss_row = jnp.sum(far_rows, axis=0, keepdims=True)
    near_rows = gathered(loss_row, near_groups(pairs, holders))
    dpo_loss = jnp.sum(near_rows, axis=0)[0]
    return ((token_grads * summed_rows).reshape(hidden.shape), dpo_loss)


def solution(mesh):
    return jax.shard_map(
        shards,
        mesh=mesh,
        in_specs=(
            P("dp", None, None, "vocab"),
            P(None, "vocab"),
            P("dp", None, None),
            P("dp", None),
            P("dp", None, None),
            P("dp", None),
            P("dp"),
            P(),
        ),
        out_specs=(P("dp", None, None, "vocab"), P()),
        check_vma=False,
    )
```

```python
import functools

import jax
import jax.numpy as jnp
from jax import lax
from jax.experimental import pallas as pl
from jax.experimental.pallas import tpu as pltpu
from jax.sharding import PartitionSpec as P

beta_scale = 0.05
both_axes = ("dp", "vocab")
cores = 2
side = 4
near_chips = 4
stat_rows = 8
closing_steps = 4
vmem_grant = 24 * 1024 * 1024


def line_groups(pairs, holders, first):
    groups = []
    for pair in range(pairs):
        along_x = (pair % cores == 0) == first
        for line in range(side):
            places = [line * side + k if along_x else k * side + line for k in range(side)]
            groups.append([pair * holders + place for place in places])
    return groups


def snake(holders):
    return [
        line * side + (k if line % 2 == 0 else side - 1 - k)
        for line in range(holders // side)
        for k in range(side)
    ]


def plane_groups(pairs, holders):
    return [[pair * holders + place for place in snake(holders)] for pair in range(pairs)]


def chip_plane_groups(pairs, holders):
    return [
        [pair * holders + place for pair in (first, first + 1) for place in range(holders)]
        for first in range(0, pairs, cores)
    ]


def near_groups(pairs, holders):
    block = cores * near_chips
    return [
        [(start + k) * holders + place for k in range(0, block, cores)]
        for first in range(0, pairs, block)
        for start in range(first, first + cores)
        for place in range(holders)
    ]


def far_groups(pairs, holders):
    block = cores * near_chips
    return [
        [(first + k) * holders + place for first in range(0, pairs, block)]
        for k in range(block)
        for place in range(holders)
    ]


def split_parts(values):
    high = values.astype(jnp.bfloat16)
    low = (values - high.astype(jnp.float32)).astype(jnp.bfloat16)
    return high, low


def stacked_parts(values):
    return jnp.concatenate(split_parts(values), axis=0)


def product(both, weight, weight_dim):
    rows = both.shape[0] // 2
    high, low = split_parts(weight)
    dims = (((1,), (weight_dim,)), ((), ()))
    wide = lax.dot_general(both, high, dims, preferred_element_type=jnp.float32)
    narrow = lax.dot_general(both[:rows], low, dims, preferred_element_type=jnp.float32)
    return wide[:rows] + (wide[rows:] + narrow)


def column_matches(target_row, base, columns):
    ids = base + lax.broadcasted_iota(jnp.int32, (columns, target_row.shape[1]), 0)
    return ids == target_row


def holder_of(block, own_core):
    return jnp.where(own_core == 0, block, (block % side) * side + block // side)


def copies_kernel(shard_ref, out_ref):
    shard = shard_ref[...]
    for k in range(out_ref.shape[0]):
        out_ref[k] = shard


def copies_for_all(shard, holders):
    return pl.pallas_call(
        copies_kernel,
        out_shape=jax.ShapeDtypeStruct((holders, *shard.shape), shard.dtype),
        in_specs=[pl.BlockSpec(memory_space=pltpu.VMEM)],
        out_specs=pl.BlockSpec(memory_space=pltpu.VMEM),
        compiler_params=pltpu.CompilerParams(vmem_limit_bytes=vmem_grant),
        name="state_copies",
    )(shard)


def token_row(values_ref):
    pairs, ones, _ = values_ref.shape
    pieces = [values_ref[pair, one : one + 1] for pair in range(pairs) for one in range(ones)]
    return jnp.concatenate(pieces, axis=1)


def logits_kernel(
    lengths_ref,
    ref_logp_ref,
    group_map_ref,
    weight_of_ref,
    targets_ref,
    rest_lse_ref,
    states_ref,
    weight_ref,
    scaled_ref,
    matches_ref,
    own_ref,
    stats_ref,
):
    pair_count, _, seq_slots = targets_ref.shape
    target_row = token_row(targets_ref)
    token = lax.broadcasted_iota(jnp.int32, target_row.shape, 1)
    slot, sequence = token % seq_slots, token // seq_slots
    group_weights = weight_of_ref[...]
    group_ids = lax.broadcasted_iota(jnp.int32, group_weights.shape, 1)
    divisor = pair_count * jnp.sum(group_weights, axis=1, keepdims=True)
    count = jnp.zeros(target_row.shape, jnp.int32)
    prior = jnp.zeros(target_row.shape, jnp.float32)
    share = jnp.zeros(target_row.shape, jnp.float32)
    for pair in range(pair_count):
        chosen_group = group_ids == group_map_ref[0:1, pair : pair + 1]
        pair_weight = jnp.sum(jnp.where(chosen_group, group_weights, 0.0), axis=1, keepdims=True)
        share = jnp.where(sequence // 2 == pair, pair_weight / divisor, share)
        for one in range(2):
            here = sequence == 2 * pair + one
            count = jnp.where(here, lengths_ref[pair : pair + 1, one : one + 1], count)
            prior = jnp.where(here, ref_logp_ref[pair : pair + 1, one : one + 1], prior)
    live = jnp.where(slot < count, 1.0, 0.0)

    own_core = lax.axis_index("dp") % cores
    total = product(stacked_parts(states_ref[0]), weight_ref[0], 0)
    for k in range(1, states_ref.shape[0]):
        total += product(stacked_parts(states_ref[k]), weight_ref[holder_of(k, own_core)], 0)
    logits = total.T
    peak = jnp.max(logits, axis=0, keepdims=True)
    scaled = jnp.exp(logits - peak)
    scaled_ref[...] = scaled
    ids = lax.axis_index("vocab") * logits.shape[0] + lax.broadcasted_iota(jnp.int32, logits.shape, 0)
    matches = ids == target_row
    matches_ref[...] = matches.astype(jnp.float32)
    exponentials = jnp.sum(scaled, axis=0, keepdims=True)
    target = jnp.sum(jnp.where(matches, logits, 0.0), axis=0, keepdims=True)
    row = lax.broadcasted_iota(jnp.int32, own_ref.shape, 0)
    stats = jnp.zeros(own_ref.shape, jnp.float32)
    for k, values in enumerate((peak, exponentials, target, token_row(rest_lse_ref), live, prior, share)):
        stats = jnp.where(row == k, values, stats)
    own_ref[...] = stats
    for k in range(stats_ref.shape[0]):
        stats_ref[k] = stats


def local_logits(small, targets, rest_lse, states, weight_blocks):
    holders, tokens, _ = states.shape
    columns = weight_blocks.shape[2]
    in_vmem = pl.BlockSpec(memory_space=pltpu.VMEM)
    return pl.pallas_call(
        logits_kernel,
        out_shape=(
            jax.ShapeDtypeStruct((columns, tokens), jnp.float32),
            jax.ShapeDtypeStruct((columns, tokens), jnp.float32),
            jax.ShapeDtypeStruct((stat_rows, tokens), jnp.float32),
            jax.ShapeDtypeStruct((cores * holders, stat_rows, tokens), jnp.float32),
        ),
        in_specs=[in_vmem] * (len(small) + 4),
        out_specs=(in_vmem,) * 4,
        compiler_params=pltpu.CompilerParams(vmem_limit_bytes=vmem_grant),
        cost_estimate=pl.CostEstimate(
            flops=6 * states.size * columns,
            bytes_accessed=4 * (states.size + weight_blocks.size),
            transcendentals=tokens * columns,
        ),
        name="local_logits",
    )(*small, targets, rest_lse, states, weight_blocks)


def softplus(values):
    small = jnp.exp(-jnp.abs(values))
    shifted = 1.0 + small
    gap = shifted - 1.0
    safe = jnp.where(gap == 0.0, 1.0, gap)
    log_shifted = jnp.where(gap == 0.0, small, jnp.log(shifted) * (small / safe))
    return jnp.maximum(values, 0.0) + log_shifted


def joined(stats):
    peaks, totals, targets = (stats[:, k : k + 1] for k in range(3))
    row_peak = jnp.max(peaks, axis=0)
    row_total = jnp.sum(totals * jnp.exp(peaks - row_peak[None]), axis=0)
    window_lse = row_peak + jnp.log(row_total)
    outside = stats[0, 3:4]
    ceiling = jnp.maximum(window_lse, outside)
    full_lse = ceiling + jnp.log(jnp.exp(window_lse - ceiling) + jnp.exp(outside - ceiling))
    return full_lse, jnp.sum(targets, axis=0)


def preference(full_lse, target_logit, live, prior, share, pair_count):
    tokens = live.shape[1]
    sequence = lax.broadcasted_iota(jnp.int32, live.shape, 1) // (tokens // (2 * pair_count))
    token_logp = live * (target_logit - full_lse)
    token_grad = jnp.zeros(live.shape, jnp.float32)
    loss = jnp.zeros((1, 1), jnp.float32)

    def of_sequence(values, here):
        return jnp.sum(jnp.where(here, values, 0.0), axis=1, keepdims=True)

    def first_of(values, here):
        return jnp.max(jnp.where(here, values, -jnp.inf), axis=1, keepdims=True)

    for pair in range(pair_count):
        chosen, rejected = (sequence == 2 * pair + one for one in range(2))
        margin = beta_scale * (
            (of_sequence(token_logp, chosen) - first_of(prior, chosen))
            - (of_sequence(token_logp, rejected) - first_of(prior, rejected))
        )
        pair_share = first_of(share, chosen)
        loss += pair_share * softplus(-margin)
        coefficient = -beta_scale * pair_share / (1.0 + jnp.exp(margin))
        token_grad += jnp.where(chosen, coefficient, 0.0) - jnp.where(rejected, coefficient, 0.0)
    return loss, live * token_grad


def rows_kernel(
    pair_count, stats_ref, own_ref, scaled_ref, matches_ref, weight_ref, rows_ref, loss_ref, grads_ref, made_ref, sems
):
    holders = weight_ref.shape[0]
    own_core = lax.axis_index("dp") % cores
    mine = pl.ds(pl.multiple_of(own_core * holders, holders), holders)
    full_lse, _ = joined(stats_ref[mine])
    scale = jnp.exp(own_ref[0:1] - full_lse)
    both = stacked_parts((matches_ref[...] - scale * scaled_ref[...]).T)
    loss = jnp.zeros((1, 1), jnp.float32)
    token_grad = jnp.zeros(loss_ref.shape, jnp.float32)
    for core in range(cores):
        stats = stats_ref[pl.ds(core * holders, holders)]
        given = (stats[0, k : k + 1] for k in range(4, 7))
        core_loss, core_grad = preference(*joined(stats), *given, pair_count)
        loss += core_loss
        token_grad = jnp.where(own_core == core, core_grad, token_grad)
    loss_ref[...] = jnp.broadcast_to(loss, loss_ref.shape)
    grads_ref[...] = jnp.broadcast_to(token_grad, grads_ref.shape[::-1]).T
    sent = []
    for k, place in enumerate(snake(holders)):
        made_ref[k] = product(both, weight_ref[place], 1)
        sent.append(pltpu.make_async_copy(made_ref.at[k], rows_ref.at[k], sems.at[k]))
        sent[k].start()
    for copy in sent:
        copy.wait()


def gradient_rows(pair_count, stats, own, scaled, matches, weight_blocks):
    holders, width, columns = weight_blocks.shape
    tokens = own.shape[1]
    rows_shape = (holders, tokens, width)
    in_vmem = pl.BlockSpec(memory_space=pltpu.VMEM)
    return pl.pallas_call(
        functools.partial(rows_kernel, pair_count),
        out_shape=(
            pltpu.HBM(rows_shape, jnp.float32),
            jax.ShapeDtypeStruct((1, tokens), jnp.float32),
            jax.ShapeDtypeStruct((tokens, width), jnp.float32),
        ),
        in_specs=[in_vmem] * 5,
        out_specs=(pl.BlockSpec(memory_space=pltpu.HBM), in_vmem, in_vmem),
        scratch_shapes=[pltpu.VMEM(rows_shape, jnp.float32), pltpu.SemaphoreType.DMA((holders,))],
        compiler_params=pltpu.CompilerParams(vmem_limit_bytes=vmem_grant),
        cost_estimate=pl.CostEstimate(
            flops=6 * tokens * weight_blocks.size,
            bytes_accessed=4 * (holders * tokens * width + weight_blocks.size),
            transcendentals=tokens * holders,
        ),
        name="gradient_rows",
    )(stats, own, scaled, matches, weight_blocks)


def closing_kernel(parts_ref, factors_ref, losses_ref, grad_ref, loss_ref, made_ref, total_ref, sems):
    total_ref[...] = jnp.sum(losses_ref[...], axis=0, keepdims=True)
    sent = [pltpu.make_async_copy(total_ref, loss_ref, sems.at[closing_steps])]
    sent[0].start()
    rows = made_ref.shape[0] // closing_steps
    for k in range(closing_steps):
        part = pl.ds(k * rows, rows)
        made_ref[part] = factors_ref[part] * jnp.sum(parts_ref[:, part], axis=0)
        sent.append(pltpu.make_async_copy(made_ref.at[part], grad_ref.at[part], sems.at[k]))
        sent[-1].start()
    for copy in sent:
        copy.wait()


def closed(parts, factors, losses):
    shape, loss_shape = factors.shape, (1, losses.shape[1])
    in_vmem = pl.BlockSpec(memory_space=pltpu.VMEM)
    in_hbm = pl.BlockSpec(memory_space=pltpu.HBM)
    return pl.pallas_call(
        closing_kernel,
        out_shape=(pltpu.HBM(shape, jnp.float32), pltpu.HBM(loss_shape, jnp.float32)),
        in_specs=[in_vmem] * 3,
        out_specs=(in_hbm, in_hbm),
        scratch_shapes=[
            pltpu.VMEM(shape, jnp.float32),
            pltpu.VMEM(loss_shape, jnp.float32),
            pltpu.SemaphoreType.DMA((closing_steps + 1,)),
        ],
        compiler_params=pltpu.CompilerParams(vmem_limit_bytes=vmem_grant),
        name="closing",
    )(parts, factors, losses)


def exchanged(blocks, groups):
    return lax.all_to_all(blocks, both_axes, 0, 0, axis_index_groups=groups, tiled=True)


def gathered(row, groups):
    return lax.all_gather(row, both_axes, axis_index_groups=groups, axis=0, tiled=True)


def shards(hidden, head_weight, targets, lengths, rest_lse, ref_logp, group_map, group_weight):
    pair_count, _, seq_slots, local_width = hidden.shape
    pairs, holders = lax.axis_size("dp"), lax.axis_size("vocab")
    tokens = pair_count * 2 * seq_slots
    weight_blocks = head_weight.reshape(holders, local_width, -1)

    first_lines = line_groups(pairs, holders, True)
    second_lines = line_groups(pairs, holders, False)

    near = exchanged(copies_for_all(hidden.reshape(tokens, local_width), side), first_lines)
    states = exchanged(jnp.broadcast_to(near, (side, *near.shape)), second_lines)
    states = states.reshape(holders, tokens, local_width)
    scaled, matches, own_stats, stat_copies = local_logits(
        (lengths, ref_logp, group_map.reshape(1, -1), group_weight.reshape(1, -1)), targets, rest_lse, states, weight_blocks
    )
    stats = exchanged(stat_copies, chip_plane_groups(pairs, holders))
    partial_rows, loss_row, token_grads = gradient_rows(
        pair_count, stats, own_stats, scaled, matches, weight_blocks
    )
    row_parts = exchanged(partial_rows, plane_groups(pairs, holders))
    far_rows = gathered(loss_row, far_groups(pairs, holders))
    loss_row = jnp.sum(far_rows, axis=0, keepdims=True)
    near_rows = gathered(loss_row, near_groups(pairs, holders))
    hidden_grad, total_row = closed(row_parts, token_grads, near_rows)
    return (hidden_grad.reshape(hidden.shape), total_row[0, 0])


def solution(mesh):
    return jax.shard_map(
        shards,
        mesh=mesh,
        in_specs=(
            P("dp", None, None, "vocab"),
            P(None, "vocab"),
            P("dp", None, None),
            P("dp", None),
            P("dp", None, None),
            P("dp", None),
            P("dp"),
            P(),
        ),
        out_specs=(P("dp", None, None, "vocab"), P()),
        check_vma=False,
    )
```

```python
import functools

import jax
import jax.numpy as jnp
from jax import lax
from jax.experimental import pallas as pl
from jax.experimental.pallas import tpu as pltpu
from jax.sharding import PartitionSpec as P

beta_scale = 0.05
both_axes = ("dp", "vocab")
cores = 2
side = 4
near_chips = 4
stat_rows = 8
closing_steps = 4
vmem_grant = 24 * 1024 * 1024


def line_groups(pairs, holders, first):
    groups = []
    for pair in range(pairs):
        along_x = (pair % cores == 0) == first
        for line in range(side):
            places = [line * side + k if along_x else k * side + line for k in range(side)]
            groups.append([pair * holders + place for place in places])
    return groups


def snake(holders):
    return [
        line * side + (k if line % 2 == 0 else side - 1 - k)
        for line in range(holders // side)
        for k in range(side)
    ]


def by_columns(holders):
    return [(place % side) * side + place // side for place in range(holders)]


def plane_groups(pairs, holders):
    orders = (snake(holders), by_columns(holders))
    return [
        [pair * holders + place for place in orders[pair % cores]] for pair in range(pairs)
    ]


def chip_plane_groups(pairs, holders):
    return [
        [pair * holders + place for pair in (first, first + 1) for place in range(holders)]
        for first in range(0, pairs, cores)
    ]


def near_groups(pairs, holders):
    block = cores * near_chips
    return [
        [(start + k) * holders + place for k in range(0, block, cores)]
        for first in range(0, pairs, block)
        for start in range(first, first + cores)
        for place in range(holders)
    ]


def far_groups(pairs, holders):
    block = cores * near_chips
    return [
        [(first + k) * holders + place for first in range(0, pairs, block)]
        for k in range(block)
        for place in range(holders)
    ]


def split_parts(values):
    high = values.astype(jnp.bfloat16)
    low = (values - high.astype(jnp.float32)).astype(jnp.bfloat16)
    return high, low


def stacked_parts(values):
    return jnp.concatenate(split_parts(values), axis=0)


def product(both, weight, weight_dim):
    rows = both.shape[0] // 2
    high, low = split_parts(weight)
    dims = (((1,), (weight_dim,)), ((), ()))
    wide = lax.dot_general(both, high, dims, preferred_element_type=jnp.float32)
    narrow = lax.dot_general(both[:rows], low, dims, preferred_element_type=jnp.float32)
    return wide[:rows] + (wide[rows:] + narrow)


def column_matches(target_row, base, columns):
    ids = base + lax.broadcasted_iota(jnp.int32, (columns, target_row.shape[1]), 0)
    return ids == target_row


def holder_of(block, own_core):
    return jnp.where(own_core == 0, block, (block % side) * side + block // side)


def copies_kernel(shard_ref, out_ref):
    shard = shard_ref[...]
    for k in range(out_ref.shape[0]):
        out_ref[k] = shard


def copies_for_all(shard, holders):
    return pl.pallas_call(
        copies_kernel,
        out_shape=jax.ShapeDtypeStruct((holders, *shard.shape), shard.dtype),
        in_specs=[pl.BlockSpec(memory_space=pltpu.VMEM)],
        out_specs=pl.BlockSpec(memory_space=pltpu.VMEM),
        compiler_params=pltpu.CompilerParams(vmem_limit_bytes=vmem_grant),
        name="state_copies",
    )(shard)


def token_row(values_ref):
    pairs, ones, _ = values_ref.shape
    pieces = [values_ref[pair, one : one + 1] for pair in range(pairs) for one in range(ones)]
    return jnp.concatenate(pieces, axis=1)


def logits_kernel(
    lengths_ref,
    ref_logp_ref,
    group_map_ref,
    weight_of_ref,
    targets_ref,
    rest_lse_ref,
    states_ref,
    weight_ref,
    scaled_ref,
    matches_ref,
    own_ref,
    stats_ref,
):
    pair_count, _, seq_slots = targets_ref.shape
    target_row = token_row(targets_ref)
    token = lax.broadcasted_iota(jnp.int32, target_row.shape, 1)
    slot, sequence = token % seq_slots, token // seq_slots
    group_weights = weight_of_ref[...]
    group_ids = lax.broadcasted_iota(jnp.int32, group_weights.shape, 1)
    divisor = pair_count * jnp.sum(group_weights, axis=1, keepdims=True)
    count = jnp.zeros(target_row.shape, jnp.int32)
    prior = jnp.zeros(target_row.shape, jnp.float32)
    share = jnp.zeros(target_row.shape, jnp.float32)
    for pair in range(pair_count):
        chosen_group = group_ids == group_map_ref[0:1, pair : pair + 1]
        pair_weight = jnp.sum(jnp.where(chosen_group, group_weights, 0.0), axis=1, keepdims=True)
        share = jnp.where(sequence // 2 == pair, pair_weight / divisor, share)
        for one in range(2):
            here = sequence == 2 * pair + one
            count = jnp.where(here, lengths_ref[pair : pair + 1, one : one + 1], count)
            prior = jnp.where(here, ref_logp_ref[pair : pair + 1, one : one + 1], prior)
    live = jnp.where(slot < count, 1.0, 0.0)

    own_core = lax.axis_index("dp") % cores
    total = product(stacked_parts(states_ref[0]), weight_ref[0], 0)
    for k in range(1, states_ref.shape[0]):
        total += product(stacked_parts(states_ref[k]), weight_ref[holder_of(k, own_core)], 0)
    logits = total.T
    peak = jnp.max(logits, axis=0, keepdims=True)
    scaled = jnp.exp(logits - peak)
    scaled_ref[...] = scaled
    ids = lax.axis_index("vocab") * logits.shape[0] + lax.broadcasted_iota(jnp.int32, logits.shape, 0)
    matches = ids == target_row
    matches_ref[...] = matches.astype(jnp.float32)
    exponentials = jnp.sum(scaled, axis=0, keepdims=True)
    target = jnp.sum(jnp.where(matches, logits, 0.0), axis=0, keepdims=True)
    row = lax.broadcasted_iota(jnp.int32, own_ref.shape, 0)
    stats = jnp.zeros(own_ref.shape, jnp.float32)
    for k, values in enumerate((peak, exponentials, target, token_row(rest_lse_ref), live, prior, share)):
        stats = jnp.where(row == k, values, stats)
    own_ref[...] = stats
    for k in range(stats_ref.shape[0]):
        stats_ref[k] = stats


def local_logits(small, targets, rest_lse, states, weight_blocks):
    holders, tokens, _ = states.shape
    columns = weight_blocks.shape[2]
    in_vmem = pl.BlockSpec(memory_space=pltpu.VMEM)
    return pl.pallas_call(
        logits_kernel,
        out_shape=(
            jax.ShapeDtypeStruct((columns, tokens), jnp.float32),
            jax.ShapeDtypeStruct((columns, tokens), jnp.float32),
            jax.ShapeDtypeStruct((stat_rows, tokens), jnp.float32),
            jax.ShapeDtypeStruct((cores * holders, stat_rows, tokens), jnp.float32),
        ),
        in_specs=[in_vmem] * (len(small) + 4),
        out_specs=(in_vmem,) * 4,
        compiler_params=pltpu.CompilerParams(vmem_limit_bytes=vmem_grant),
        cost_estimate=pl.CostEstimate(
            flops=6 * states.size * columns,
            bytes_accessed=4 * (states.size + weight_blocks.size),
            transcendentals=tokens * columns,
        ),
        name="local_logits",
    )(*small, targets, rest_lse, states, weight_blocks)


def softplus(values):
    small = jnp.exp(-jnp.abs(values))
    shifted = 1.0 + small
    gap = shifted - 1.0
    safe = jnp.where(gap == 0.0, 1.0, gap)
    log_shifted = jnp.where(gap == 0.0, small, jnp.log(shifted) * (small / safe))
    return jnp.maximum(values, 0.0) + log_shifted


def joined(stats):
    peaks, totals, targets = (stats[:, k : k + 1] for k in range(3))
    row_peak = jnp.max(peaks, axis=0)
    row_total = jnp.sum(totals * jnp.exp(peaks - row_peak[None]), axis=0)
    window_lse = row_peak + jnp.log(row_total)
    outside = stats[0, 3:4]
    ceiling = jnp.maximum(window_lse, outside)
    full_lse = ceiling + jnp.log(jnp.exp(window_lse - ceiling) + jnp.exp(outside - ceiling))
    return full_lse, jnp.sum(targets, axis=0)


def preference(full_lse, target_logit, live, prior, share, pair_count):
    tokens = live.shape[1]
    sequence = lax.broadcasted_iota(jnp.int32, live.shape, 1) // (tokens // (2 * pair_count))
    token_logp = live * (target_logit - full_lse)
    token_grad = jnp.zeros(live.shape, jnp.float32)
    loss = jnp.zeros((1, 1), jnp.float32)

    def of_sequence(values, here):
        return jnp.sum(jnp.where(here, values, 0.0), axis=1, keepdims=True)

    def first_of(values, here):
        return jnp.max(jnp.where(here, values, -jnp.inf), axis=1, keepdims=True)

    for pair in range(pair_count):
        chosen, rejected = (sequence == 2 * pair + one for one in range(2))
        margin = beta_scale * (
            (of_sequence(token_logp, chosen) - first_of(prior, chosen))
            - (of_sequence(token_logp, rejected) - first_of(prior, rejected))
        )
        pair_share = first_of(share, chosen)
        loss += pair_share * softplus(-margin)
        coefficient = -beta_scale * pair_share / (1.0 + jnp.exp(margin))
        token_grad += jnp.where(chosen, coefficient, 0.0) - jnp.where(rejected, coefficient, 0.0)
    return loss, live * token_grad


def rows_kernel(
    pair_count, stats_ref, own_ref, scaled_ref, matches_ref, weight_ref, rows_ref, loss_ref, grads_ref, made_ref, sems
):
    holders = weight_ref.shape[0]
    own_core = lax.axis_index("dp") % cores
    mine = pl.ds(pl.multiple_of(own_core * holders, holders), holders)
    full_lse, _ = joined(stats_ref[mine])
    scale = jnp.exp(own_ref[0:1] - full_lse)
    both = stacked_parts((matches_ref[...] - scale * scaled_ref[...]).T)
    loss = jnp.zeros((1, 1), jnp.float32)
    token_grad = jnp.zeros(loss_ref.shape, jnp.float32)
    for core in range(cores):
        stats = stats_ref[pl.ds(core * holders, holders)]
        given = (stats[0, k : k + 1] for k in range(4, 7))
        core_loss, core_grad = preference(*joined(stats), *given, pair_count)
        loss += core_loss
        token_grad = jnp.where(own_core == core, core_grad, token_grad)
    loss_ref[...] = jnp.broadcast_to(loss, loss_ref.shape)
    grads_ref[...] = jnp.broadcast_to(token_grad, grads_ref.shape[::-1]).T
    sent = []
    for k, (even, odd) in enumerate(zip(snake(holders), by_columns(holders))):
        made_ref[k] = product(both, weight_ref[jnp.where(own_core == 0, even, odd)], 1)
        sent.append(pltpu.make_async_copy(made_ref.at[k], rows_ref.at[k], sems.at[k]))
        sent[k].start()
    for copy in sent:
        copy.wait()


def gradient_rows(pair_count, stats, own, scaled, matches, weight_blocks):
    holders, width, columns = weight_blocks.shape
    tokens = own.shape[1]
    rows_shape = (holders, tokens, width)
    in_vmem = pl.BlockSpec(memory_space=pltpu.VMEM)
    return pl.pallas_call(
        functools.partial(rows_kernel, pair_count),
        out_shape=(
            pltpu.HBM(rows_shape, jnp.float32),
            jax.ShapeDtypeStruct((1, tokens), jnp.float32),
            jax.ShapeDtypeStruct((tokens, width), jnp.float32),
        ),
        in_specs=[in_vmem] * 5,
        out_specs=(pl.BlockSpec(memory_space=pltpu.HBM), in_vmem, in_vmem),
        scratch_shapes=[pltpu.VMEM(rows_shape, jnp.float32), pltpu.SemaphoreType.DMA((holders,))],
        compiler_params=pltpu.CompilerParams(vmem_limit_bytes=vmem_grant),
        cost_estimate=pl.CostEstimate(
            flops=6 * tokens * weight_blocks.size,
            bytes_accessed=4 * (holders * tokens * width + weight_blocks.size),
            transcendentals=tokens * holders,
        ),
        name="gradient_rows",
    )(stats, own, scaled, matches, weight_blocks)


def closing_kernel(parts_ref, factors_ref, losses_ref, grad_ref, loss_ref, made_ref, total_ref, sems):
    total_ref[...] = jnp.sum(losses_ref[...], axis=0, keepdims=True)
    sent = [pltpu.make_async_copy(total_ref, loss_ref, sems.at[closing_steps])]
    sent[0].start()
    rows = made_ref.shape[0] // closing_steps
    for k in range(closing_steps):
        part = pl.ds(k * rows, rows)
        made_ref[part] = factors_ref[part] * jnp.sum(parts_ref[:, part], axis=0)
        sent.append(pltpu.make_async_copy(made_ref.at[part], grad_ref.at[part], sems.at[k]))
        sent[-1].start()
    for copy in sent:
        copy.wait()


def closed(parts, factors, losses):
    shape, loss_shape = factors.shape, (1, losses.shape[1])
    in_vmem = pl.BlockSpec(memory_space=pltpu.VMEM)
    in_hbm = pl.BlockSpec(memory_space=pltpu.HBM)
    return pl.pallas_call(
        closing_kernel,
        out_shape=(pltpu.HBM(shape, jnp.float32), pltpu.HBM(loss_shape, jnp.float32)),
        in_specs=[in_vmem] * 3,
        out_specs=(in_hbm, in_hbm),
        scratch_shapes=[
            pltpu.VMEM(shape, jnp.float32),
            pltpu.VMEM(loss_shape, jnp.float32),
            pltpu.SemaphoreType.DMA((closing_steps + 1,)),
        ],
        compiler_params=pltpu.CompilerParams(vmem_limit_bytes=vmem_grant),
        name="closing",
    )(parts, factors, losses)


def exchanged(blocks, groups):
    return lax.all_to_all(blocks, both_axes, 0, 0, axis_index_groups=groups, tiled=True)


def gathered(row, groups):
    return lax.all_gather(row, both_axes, axis_index_groups=groups, axis=0, tiled=True)


def shards(hidden, head_weight, targets, lengths, rest_lse, ref_logp, group_map, group_weight):
    pair_count, _, seq_slots, local_width = hidden.shape
    pairs, holders = lax.axis_size("dp"), lax.axis_size("vocab")
    tokens = pair_count * 2 * seq_slots
    weight_blocks = head_weight.reshape(holders, local_width, -1)

    first_lines = line_groups(pairs, holders, True)
    second_lines = line_groups(pairs, holders, False)

    near = exchanged(copies_for_all(hidden.reshape(tokens, local_width), side), first_lines)
    states = exchanged(jnp.broadcast_to(near, (side, *near.shape)), second_lines)
    states = states.reshape(holders, tokens, local_width)
    scaled, matches, own_stats, stat_copies = local_logits(
        (lengths, ref_logp, group_map.reshape(1, -1), group_weight.reshape(1, -1)), targets, rest_lse, states, weight_blocks
    )
    stats = exchanged(stat_copies, chip_plane_groups(pairs, holders))
    partial_rows, loss_row, token_grads = gradient_rows(
        pair_count, stats, own_stats, scaled, matches, weight_blocks
    )
    row_parts = exchanged(partial_rows, plane_groups(pairs, holders))
    far_rows = gathered(loss_row, far_groups(pairs, holders))
    loss_row = jnp.sum(far_rows, axis=0, keepdims=True)
    near_rows = gathered(loss_row, near_groups(pairs, holders))
    hidden_grad, total_row = closed(row_parts, token_grads, near_rows)
    return (hidden_grad.reshape(hidden.shape), total_row[0, 0])


def solution(mesh):
    return jax.shard_map(
        shards,
        mesh=mesh,
        in_specs=(
            P("dp", None, None, "vocab"),
            P(None, "vocab"),
            P("dp", None, None),
            P("dp", None),
            P("dp", None, None),
            P("dp", None),
            P("dp"),
            P(),
        ),
        out_specs=(P("dp", None, None, "vocab"), P()),
        check_vma=False,
    )
```
